32 devices in a mesh: dp: 2 (over x), expert: 16 (over z, y, core).
Axes of the slice: x: 2, y: 2, z: 4, core: 2. Of those that a mesh axis runs over, the one named last changes fastest.
Arguments:
- cotangent: bfloat16 [4096, 3584], P(('dp', 'expert')), may hold values from -0.59765625 to 0.59765625
- expert_ids: int32 [4096, 1], P(('dp', 'expert')), may hold values from 0 to 3; in each aligned block of 128 rows (0 to 127, 128 to 255, ...) at most 48 rows name the same one
- route_weights: float32 [4096, 1], P(('dp', 'expert')), may hold values from 0.1 to 1
- gate_pre: bfloat16 [1536, 4096], P('dp', 'expert'), may hold values from -5 to 5
- up_pre: bfloat16 [1536, 4096], P('dp', 'expert'), may hold values from -5 to 5
- down_weight: bfloat16 [3584, 4096], P('dp', 'expert'), may hold values from -0.1875 to 0.1875
Outputs:
- weight_grad: bfloat16 [3584, 4096], P('dp', 'expert')
- gate_grad: bfloat16 [1536, 4096], P('dp', 'expert')
- up_grad: bfloat16 [1536, 4096], P('dp', 'expert')
The draws below stay inside these ranges and needn't reach their ends.
Inputs may be any that keep to these rules, and one draw needn't show every extreme that they name: `expert_ids`: each token names one expert. Among the tokens of one device, at most 48 name the same expert, and in every draw some expert is named by exactly 48 tokens of some device.
All inputs are finite; a program needn't handle non-finite values.
Results may differ from the reference program's by a relative error of at most 0.013.
Values may be sent and summed in bfloat16 or wider, within the bound.
A program may use at most 64 MiB of HBM per device.

```python
import math
import jax
import jax.numpy as jnp
import numpy as np
from jax import lax

D = 3584
FFW = 1024
TOP = 1
TOK_DEV = 128
EXPERTS = 4
CAP = 48
TOKENS = 4096
SLOTS = 1536
N_DP = 2
N_EXPERT = 16


def shard_levels(own_key, extent, split, low, largest):
    def one(axis_at, parts):
        steps = jax.random.uniform(jax.random.fold_in(jax.random.fold_in(own_key, 6), axis_at), (parts,), jnp.float32, low / len(split), largest / len(split))
        return jnp.repeat(jnp.exp(steps), extent[axis_at] // parts).reshape((-1,) + (1,) * (len(extent) - axis_at - 1))

    gain = one(*split[0])
    for cut in split[1:]:
        gain = gain * one(*cut)
    return gain


def assign_block(own_key, own, number, rows, count, top, limit, skew):
    order = jax.random.permutation(own_key, count)
    heavy_load, common = load_shares(count, rows * top, limit, skew, True), load_shares(count, rows * top, limit, skew, False)
    places = jnp.arange(count)

    def named(lengths, turn):
        used = int((lengths > 0).sum())
        fixed = max(1, used // 4)
        shifted = fixed + (places - fixed + turn * (used - fixed)) % max(1, count - fixed)
        return jnp.zeros((count,), jnp.int32).at[order[jnp.where(places < fixed, places, shifted)]].set(jnp.asarray(lengths, jnp.int32))

    lengths = jnp.where(number % 4 == 0, named(heavy_load, number // 4), named(common, number - number // 4 - 1))
    mixed = jax.random.permutation(jax.random.fold_in(own, 3), count)
    source_of, receiver = mixed[0:count // 2 * 2:2], mixed[1:count // 2 * 2:2]
    room = jnp.minimum(lengths[source_of] - 1, limit - lengths[receiver]) // 2
    room = jnp.where((source_of == order[0]) | (receiver == order[0]) | (lengths[receiver] == 0), 0, jnp.maximum(room, 0))
    shifted = jax.random.randint(jax.random.fold_in(own, 4), (count // 2,), 0, 1 << 20) % (room + 1)
    lengths = lengths.at[source_of].add(-shifted).at[receiver].add(shifted)
    labels = jnp.searchsorted(jnp.cumsum(lengths), jnp.arange(rows * top), side="right").astype(jnp.int32)
    listing = labels.reshape(top, rows).T
    listing = listing[jax.random.permutation(jax.random.fold_in(own, 1), rows)]
    turn = jax.random.randint(jax.random.fold_in(own, 2), (rows, 1), 0, top)
    return jnp.take_along_axis(listing, (jnp.arange(top)[None, :] + turn) % top, axis=1)


def load_shares(count, total, most, lean, full):
    weights = [(1 << 20) // math.isqrt(standing ** lean) + 1 for standing in range(1, count + 1)]
    largest = most if full else min(most, max(-(-total // count), total * weights[0] // sum(weights)))
    least = 1 if total - largest >= count - 1 else 0
    holding, surplus = [largest] + [least] * (count - 1), total - largest - least * (count - 1)
    while surplus > 0:
        movable = [i for i in range(1, count) if holding[i] < largest] or [i for i in range(1, count) if holding[i] < most]
        whole, left = sum([weights[i] for i in movable]), surplus
        for i in movable:
            more = min(most - holding[i], max(1, left * weights[i] // whole), surplus)
            holding[i] = holding[i] + more
            surplus = surplus - more
    return np.array(holding)


def normal_values(rng, extent, width, limit, cuts=(), kind=jnp.bfloat16):
    drawn = width * jax.random.normal(rng, extent, jnp.float32)
    if cuts:
        drawn = drawn * shard_levels(rng, extent, cuts, -0.22, 0.18)
    return jnp.clip(drawn, -limit, limit).astype(kind)


def setup_inputs(seed: int = 0) -> dict:
    splits = jax.random.split(jax.random.key(seed), 7)
    cotangent = normal_values(splits[0], (TOKENS, D), 0.1, 0.59765625, ((0, 32),))
    expert_ids_keys = jax.random.split(jax.random.fold_in(splits[1], 1), TOKENS // TOK_DEV)
    expert_ids_turns = jax.random.permutation(jax.random.fold_in(splits[1], 3), TOKENS // TOK_DEV)
    expert_ids = jax.vmap(lambda own, number: assign_block(jax.random.fold_in(splits[1], 2), own, number, TOK_DEV, EXPERTS, TOP, CAP, 2))(expert_ids_keys, expert_ids_turns).reshape((TOKENS, TOP))
    route_weights = jnp.clip(0.1 + 0.9 * jax.random.uniform(splits[2], (TOKENS, TOP), jnp.float32) ** shard_levels(splits[2], (TOKENS, TOP), ((0, 32),), -0.2, 0.2), 0.1, 1.0)
    gate_pre = normal_values(splits[3], (SLOTS, EXPERTS * FFW), 1.0, 5.0, ((0, 2), (1, 16)))
    up_pre = normal_values(splits[4], (SLOTS, EXPERTS * FFW), 1.0, 5.0, ((0, 2), (1, 16)))
    down_weight = normal_values(splits[5], (D, EXPERTS * FFW), FFW ** -0.5, 0.1875, ((0, 2), (1, 16)))
    return {"cotangent": cotangent, "expert_ids": expert_ids, "route_weights": route_weights, "gate_pre": gate_pre, "up_pre": up_pre, "down_weight": down_weight}


def group_terms(cotangent, expert_ids, route_weights, gate_pre, up_pre, down_weight):
    onehot = (expert_ids[..., None] == jnp.arange(EXPERTS, dtype=jnp.int32)).astype(jnp.int32)
    touched = jnp.sum(onehot, axis=2)
    earlier = jnp.cumsum(touched, axis=1) - touched
    position = jnp.sum(onehot * earlier[:, :, None, :], axis=3)
    sources = jnp.arange(N_EXPERT, dtype=jnp.int32)[:, None, None] * CAP
    rows = (sources + position).astype(jnp.int32)
    scaled = route_weights[..., None] * cotangent.astype(jnp.float32)[:, :, None, :]
    routed = jnp.zeros((EXPERTS, N_EXPERT * CAP, D), jnp.float32).at[expert_ids, rows].add(scaled)
    routed_half = lax.optimization_barrier(routed.astype(jnp.bfloat16))
    routed_full = routed_half.astype(jnp.float32)
    weights = down_weight.astype(jnp.float32).reshape(D, EXPERTS, FFW)
    gate_full = gate_pre.astype(jnp.float32).reshape(N_EXPERT * CAP, EXPERTS, FFW)
    up_full = up_pre.astype(jnp.float32).reshape(N_EXPERT * CAP, EXPERTS, FFW)
    upstream = jnp.einsum('xrd,dxf->rxf', routed_full, weights)
    sigmoid = jax.nn.sigmoid(gate_full)
    active = gate_full * sigmoid
    product_half = lax.optimization_barrier((active * up_full).astype(jnp.bfloat16))
    gate_grad = (upstream * up_full * sigmoid * (1.0 + gate_full * (1.0 - sigmoid))).astype(jnp.bfloat16)
    up_grad = (upstream * active).astype(jnp.bfloat16)
    partial_sum = jnp.einsum('xrd,rxf->dxf', routed_full, product_half.astype(jnp.float32))
    partial_half = partial_sum.reshape(D, EXPERTS * FFW).astype(jnp.bfloat16)
    return partial_half, gate_grad.reshape(N_EXPERT * CAP, EXPERTS * FFW), up_grad.reshape(N_EXPERT * CAP, EXPERTS * FFW)


def reference(cotangent, expert_ids, route_weights, gate_pre, up_pre, down_weight):
    stacked = (cotangent.reshape(N_DP, N_EXPERT, TOK_DEV, D),
               expert_ids.reshape(N_DP, N_EXPERT, TOK_DEV, TOP),
               route_weights.reshape(N_DP, N_EXPERT, TOK_DEV, TOP),
               gate_pre.reshape(N_DP, N_EXPERT * CAP, EXPERTS * FFW),
               up_pre.reshape(N_DP, N_EXPERT * CAP, EXPERTS * FFW))

    def step(total, pieces):
        partial_half, gate_grad, up_grad = group_terms(pieces[0], pieces[1], pieces[2], pieces[3], pieces[4], down_weight)
        return total + partial_half.astype(jnp.float32), (gate_grad, up_grad)

    start = jnp.zeros((D, EXPERTS * FFW), jnp.float32)
    total, grads = lax.scan(step, start, stacked)
    weight_grad = total.astype(jnp.bfloat16)
    gate_grad = grads[0].reshape(SLOTS, EXPERTS * FFW)
    up_grad = grads[1].reshape(SLOTS, EXPERTS * FFW)
    return weight_grad, gate_grad, up_grad
```

```python
import functools

import jax
import jax.numpy as jnp
from jax import lax
from jax.experimental import pallas as pl
from jax.experimental.pallas import tpu as pltpu
from jax.sharding import PartitionSpec as P

SPLIT = 4
EARLY = 2
BUILD = 3
LAG = 2


def kernel(
    sizes,
    cot_hbm,
    ids_hbm,
    weights_hbm,
    gate_hbm,
    up_hbm,
    down_hbm,
    wgrad_ref,
    ggrad_ref,
    ugrad_ref,
    cot_ref,
    ids_ref,
    weights_ref,
    gate_ref,
    up_ref,
    down_ref,
    load,
    sendbuf,
    routed,
    cot_in,
    ids_in,
    weights_in,
    up_out,
    up_in,
    upstream,
    slope,
    active,
    product,
    picker,
    scale,
    z_send,
    z_recv,
    y_send,
    y_recv,
    c_send,
    c_recv,
    x_send,
    x_recv,
    i_send,
    i_recv,
    p_send,
    p_recv,
    u_send,
    u_recv,
):
    n, experts, cap, chunks, width, aligned = sizes
    own = chunks // n
    away = chunks - own
    early = min(EARLY, own - 1)
    ahead = min(BUILD, chunks)
    tokens = ids_ref.shape[1]
    dp = lax.axis_index("dp")
    me = lax.axis_index("expert")
    e, lane = me // SPLIT, me % SPLIT
    across = me - lane + (lane + 2) % SPLIT
    beside = me - lane + (lane // 2) * 2 + (lane + 1) % 2
    lane_across = (lane + 2) % SPLIT

    loads = [
        pltpu.make_async_copy(source, to, load.at[i])
        for i, (source, to) in enumerate(
            (
                (cot_hbm, cot_ref),
                (gate_hbm, gate_ref),
                (up_hbm, up_ref),
                (down_hbm, down_ref),
                (ids_hbm, ids_ref),
                (weights_hbm, weights_ref),
            )
        )
    ]
    for i in (4, 5, 0, 1, 2, 3):
        loads[i].start()

    barrier = pltpu.get_barrier_semaphore()

    def greet(target):
        pl.semaphore_signal(
            barrier, inc=1, device_id=target, device_id_type=pl.DeviceIdType.MESH
        )

    for k in range(1, experts):
        greet({"expert": (e + k) % experts * SPLIT + lane})
    greet({"expert": across})
    greet({"expert": beside})
    for k in range(1, n):
        greet({"dp": (dp + k) % n})

    def send(source, to, sent, arrived, device):
        return pltpu.make_async_remote_copy(
            src_ref=source,
            dst_ref=to,
            send_sem=sent,
            recv_sem=arrived,
            device_id=device,
            device_id_type=pl.DeviceIdType.MESH,
        )

    def chunk_at(t):
        late = jnp.where(t < early + away, own - early, -away)
        return t + jnp.where(t < early, 0, late)

    def columns_of(share, j):
        if aligned:
            return cot_ref.at[:, pl.ds(pl.multiple_of((share * own + j) * width, 128), width)]
        return cot_ref.at[share * own + j]

    def cot_copy(i):
        to = (dp - 1 - i // own + n) % n
        return send(columns_of(to, i % own), cot_in.at[i], x_send.at[0], x_recv.at[i], {"dp": to})

    def ids_copy(k):
        return send(
            ids_ref, ids_in.at[k - 1], i_send.at[k - 1, 0], i_recv.at[k - 1, 0], {"dp": (dp - k + n) % n}
        )

    def weights_copy(k):
        return send(
            weights_ref, weights_in.at[k - 1], i_send.at[k - 1, 1], i_recv.at[k - 1, 1], {"dp": (dp - k + n) % n}
        )

    def product_copy(k):
        return send(
            product.at[0], product.at[k], p_send.at[k - 1], p_recv.at[k - 1], {"dp": (dp - k + n) % n}
        )

    def up_copy(i):
        return send(up_out.at[i], up_in.at[i], u_send.at[i], u_recv.at[i], {"dp": (dp + 1 + i) % n})

    def pick(k, ids_row, weight_row):
        shape = (tokens, tokens)
        first = lax.broadcasted_iota(jnp.int32, shape, 0)
        second = lax.broadcasted_iota(jnp.int32, shape, 1)
        names = lax.broadcasted_iota(jnp.int32, (-(-experts // 16) * 16, tokens), 0) == ids_row
        before = jnp.where(first < second, 1.0, 0.0).astype(jnp.bfloat16)
        earlier = jnp.dot(
            jnp.where(names, 1.0, 0.0).astype(jnp.bfloat16), before, preferred_element_type=jnp.float32
        )
        position = jnp.sum(jnp.where(names, earlier, 0.0), axis=0, keepdims=True).astype(jnp.int32)
        target = ids_row * cap + position
        chosen = lax.broadcasted_iota(jnp.int32, (experts * cap, tokens), 0) == target
        picker[k] = jnp.where(chosen, 1.0, 0.0).astype(jnp.bfloat16)
        scale[k] = jnp.sum(jnp.where(chosen, weight_row, 0.0), axis=1, keepdims=True)

    def place(q, k, columns):
        picked = jnp.dot(picker[k], columns, preferred_element_type=jnp.float32)
        rows = (picked * scale[k]).astype(jnp.bfloat16).reshape(experts, cap, width)
        sendbuf[q] = rows
        routed[q, e, lane] = sendbuf[q, e]

    def build(t):
        q = chunk_at(t)

        @pl.when(q < own)
        def _():
            place(q, 0, columns_of(dp, q)[...])

        @pl.when(q >= own)
        def _():
            cot_copy(q - own).wait_recv()
            place(q, q // own, cot_in[q - own])

    def from_source(q, source):
        at = routed.at[q, source, lane]
        return send(at, at, y_send.at[0], y_recv.at[q], {"expert": across})

    def to_expert(t):
        q = chunk_at(t)
        for k in range(1, experts):
            there = (e + k) % experts
            send(
                sendbuf.at[q, there],
                routed.at[q, e, lane],
                z_send.at[0],
                z_recv.at[q],
                {"expert": there * SPLIT + lane},
            ).start()
        from_source(q, e).start()

    def over_y(q):
        at = routed.at[q, :, lane]
        return send(at, at, y_send.at[0], y_recv.at[q], {"expert": across})

    def over_core(q, turn):
        at = routed.at[q, :, lane if turn == 0 else lane_across]
        return send(at, at, c_send.at[0], c_recv.at[q], {"expert": beside})

    def all_of(ref_at, sem):
        pltpu.make_async_copy(ref_at, ref_at, sem).wait()

    loads[4].wait()
    loads[5].wait()
    pick(0, ids_ref[...], weights_ref[...])
    loads[0].wait()
    for j in range(early):
        place(j, 0, columns_of(dp, j)[...])
    pl.semaphore_wait(barrier, experts - 1 + 2 + n - 1)
    for k in range(1, n):
        ids_copy(k).start()
        weights_copy(k).start()

    @pl.loop(0, away)
    def _(i):
        cot_copy(i).start()

    for j in range(early):
        to_expert(j)

    rows_all = gate_ref.shape[0]
    piece = rows_all // 8
    loads[1].wait()
    loads[2].wait()

    @pl.loop(0, 8)
    def _(i):
        at = pl.ds(pl.multiple_of(i * piece, 16), piece)
        gate = gate_ref[at, :].astype(jnp.float32)
        up = up_ref[at, :].astype(jnp.float32)
        sig = jax.nn.sigmoid(gate)
        act = gate * sig
        active[at, :] = act
        slope[at, :] = up * sig * (1.0 + gate * (1.0 - sig))
        product[0, at, :] = (act * up).astype(jnp.bfloat16)
        for k in range(n):
            upstream[k, at, :] = jnp.zeros_like(act)

    for k in range(1, n):
        ids_copy(k).wait_recv()
        weights_copy(k).wait_recv()
        pick(k, ids_in[k - 1], weights_in[k - 1])
    for t in range(early, ahead):
        build(t)
    for t in range(early, ahead - 1):
        to_expert(t)
    for k in range(1, n):
        product_copy(k).start()
    loads[3].wait()

    def gradient(j):
        total = jnp.zeros((width, product.shape[2]), jnp.float32)
        for k in range(n):
            rows = routed[k * own + j].reshape(rows_all, width)
            total = total + lax.dot_general(
                rows, product[k], (((0,), (0,)), ((), ())), preferred_element_type=jnp.float32
            )
        wgrad_ref[j] = total.astype(jnp.bfloat16)

    @pl.loop(0, chunks + LAG + 1)
    def _(t):
        @pl.when(t + ahead < chunks)
        def _():
            build(t + ahead)

        @pl.when(t + ahead - 1 < chunks)
        def _():
            to_expert(t + ahead - 1)

        @pl.when(t < chunks)
        def _():
            q = chunk_at(t)
            all_of(routed.at[q, pl.ds(0, experts - 1), 0], z_recv.at[q])
            for k in range(1, experts):
                from_source(q, (e + k) % experts).start()
            over_core(q, 0).start()

        @pl.when((t >= LAG) & (t < chunks + LAG))
        def _():
            q = chunk_at(t - LAG)
            over_y(q).wait_recv()
            over_core(q, 1).start()

        @pl.when(t >= LAG + 1)
        def _():
            turn = t - LAG - 1
            q = chunk_at(turn)
            k, j = q // own, q % own
            all_of(routed.at[q, :, pl.ds(0, 2)], c_recv.at[q])
            rows = routed[q].reshape(rows_all, width)
            upstream[k] += jnp.dot(rows, down_ref[j], preferred_element_type=jnp.float32)

            @pl.when((k >= 1) & (j == own - 1))
            def _():
                up_out[k - 1] = upstream[k].astype(jnp.bfloat16)

            @pl.when(turn == early + away)
            def _():
                for i in range(1, n):
                    product_copy(i).wait_recv()
                for i in range(early):
                    gradient(i)

            @pl.when(turn >= early + away)
            def _():
                gradient(j)

            @pl.when((k >= 1) & (j == own - 1))
            def _():
                up_copy(k - 1).start()

    for k in range(1, n):
        up_copy(k - 1).wait_recv()

    @pl.loop(0, 8)
    def _(i):
        at = pl.ds(pl.multiple_of(i * piece, 16), piece)
        total = upstream[0, at, :]
        for k in range(1, n):
            total = total + up_in[k - 1, at, :].astype(jnp.float32)
        ggrad_ref[at, :] = (total * slope[at, :]).astype(jnp.bfloat16)
        ugrad_ref[at, :] = (total * active[at, :]).astype(jnp.bfloat16)

    all_of(sendbuf.at[:, pl.ds(0, experts - 1)], z_send.at[0])
    all_of(sendbuf, y_send.at[0])
    all_of(routed.at[:, :, pl.ds(0, 2)], c_send.at[0])
    all_of(cot_in, x_send.at[0])
    for k in range(1, n):
        ids_copy(k).wait_send()
        weights_copy(k).wait_send()
        product_copy(k).wait_send()
        up_copy(k - 1).wait_send()


def store(*refs):
    count = len(refs) // 2
    copies = [pltpu.make_async_copy(refs[i], refs[count + i], refs[-1].at[i]) for i in range(count)]
    for copy in copies:
        copy.start()
    for copy in copies:
        copy.wait()


def chunk_width(depth):
    for width in (256, 128):
        if depth % width == 0:
            return width, True
    return depth, False


def per_device(cotangent, expert_ids, route_weights, gate_pre, up_pre, down_weight):
    n = lax.axis_size("dp")
    devices = lax.axis_size("expert")
    experts = devices // SPLIT
    rows, hidden = gate_pre.shape
    capacity = rows // devices
    cap = -(-capacity // 16) * 16
    depth = down_weight.shape[0]
    width, aligned = chunk_width(depth)
    own = depth // width
    chunks = n * own
    away = chunks - own
    if not aligned:
        cotangent = cotangent.reshape(-1, chunks, width).swapaxes(0, 1)

    def widen(a):
        if cap == capacity:
            return a
        a = a.reshape(devices, capacity, hidden)
        return jnp.pad(a, ((0, 0), (0, cap - capacity), (0, 0))).reshape(devices * cap, hidden)

    def narrow(a):
        if cap == capacity:
            return a
        return a.reshape(devices, cap, hidden)[:, :capacity].reshape(rows, hidden)

    padded = devices * cap
    tokens = expert_ids.shape[0]
    half, full = jnp.bfloat16, jnp.float32
    vmem = pl.BlockSpec(memory_space=pltpu.VMEM)
    anywhere = pl.BlockSpec(memory_space=pltpu.HBM)
    dma = pltpu.SemaphoreType.DMA
    weight_grad, gate_grad, up_grad = pl.pallas_call(
        functools.partial(kernel, (n, experts, cap, chunks, width, aligned)),
        out_shape=(
            pltpu.VMEM((own, width, hidden), half),
            pltpu.VMEM((padded, hidden), half),
            pltpu.VMEM((padded, hidden), half),
        ),
        in_specs=[anywhere] * 6,
        out_specs=(vmem, vmem, vmem),
        scratch_shapes=[
            pltpu.VMEM(cotangent.shape, half),
            pltpu.VMEM((1, tokens), jnp.int32),
            pltpu.VMEM((1, tokens), full),
            pltpu.VMEM((padded, hidden), half),
            pltpu.VMEM((padded, hidden), half),
            pltpu.VMEM((own, width, hidden), half),
            dma((6,)),
            pltpu.VMEM((chunks, experts, cap, width), half),
            pltpu.VMEM((chunks, experts, SPLIT, cap, width), half),
            pltpu.VMEM((away, tokens, width), half),
            pltpu.VMEM((n - 1, 1, tokens), jnp.int32),
            pltpu.VMEM((n - 1, 1, tokens), full),
            pltpu.VMEM((n - 1, padded, hidden), half),
            pltpu.VMEM((n - 1, padded, hidden), half),
            pltpu.VMEM((n, padded, hidden), full),
            pltpu.VMEM((padded, hidden), full),
            pltpu.VMEM((padded, hidden), full),
            pltpu.VMEM((n, padded, hidden), half),
            pltpu.VMEM((n, experts * cap, tokens), half),
            pltpu.VMEM((n, experts * cap, 1), full),
            dma((1,)),
            dma((chunks,)),
            dma((1,)),
            dma((chunks,)),
            dma((1,)),
            dma((chunks,)),
            dma((1,)),
            dma((away,)),
            dma((n - 1, 2)),
            dma((n - 1, 2)),
            dma((n - 1,)),
            dma((n - 1,)),
            dma((n - 1,)),
            dma((n - 1,)),
        ],
        compiler_params=pltpu.CompilerParams(collective_id=0, has_side_effects=True),
    )(
        cotangent,
        expert_ids.reshape(1, -1),
        route_weights.reshape(1, -1),
        widen(gate_pre),
        widen(up_pre),
        down_weight.reshape(own, width, hidden),
    )
    results = (weight_grad.reshape(depth, hidden), gate_grad, up_grad)
    weight_grad, gate_grad, up_grad = pl.pallas_call(
        store,
        out_shape=[jax.ShapeDtypeStruct(a.shape, a.dtype) for a in results],
        in_specs=[vmem] * len(results),
        out_specs=[anywhere] * len(results),
        scratch_shapes=[dma((len(results),))],
        compiler_params=pltpu.CompilerParams(vmem_limit_bytes=1 << 22),
    )(*results)
    return weight_grad, narrow(gate_grad), narrow(up_grad)


def solution(mesh):
    placed = (
        P(("dp", "expert"), None),
        P(("dp", "expert"), None),
        P(("dp", "expert"), None),
        P("dp", "expert"),
        P("dp", "expert"),
        P("dp", "expert"),
    )
    return jax.shard_map(
        per_device,
        mesh=mesh,
        in_specs=placed,
        out_specs=(P("dp", "expert"), P("dp", "expert"), P("dp", "expert")),
        check_vma=False,
    )
```

```python
import functools

import jax
import jax.numpy as jnp
from jax import lax
from jax.experimental import pallas as pl
from jax.experimental.pallas import tpu as pltpu
from jax.sharding import PartitionSpec as P

SPLIT = 4
EARLY = 2
BUILD = 3
LAG = 2


def kernel(
    sizes,
    cot_hbm,
    ids_hbm,
    weights_hbm,
    gate_hbm,
    up_hbm,
    down_hbm,
    wgrad_ref,
    ggrad_ref,
    ugrad_ref,
    cot_ref,
    ids_ref,
    weights_ref,
    gate_ref,
    up_ref,
    down_ref,
    load,
    sendbuf,
    routed,
    cot_in,
    ids_in,
    weights_in,
    up_out,
    up_in,
    upstream,
    slope,
    active,
    product,
    picker,
    scale,
    z_send,
    z_recv,
    y_send,
    y_recv,
    c_send,
    c_recv,
    x_send,
    x_recv,
    i_send,
    i_recv,
    p_send,
    p_recv,
    u_send,
    u_recv,
):
    n, experts, cap, chunks, width, aligned = sizes
    own = chunks // n
    away = chunks - own
    early = min(EARLY, own - 1)
    ahead = min(BUILD, chunks)
    home_turn = max(0, early + away - ahead) + 1
    block = SPLIT * cap
    final = chunks - 1
    rush = early + away + 1
    steady = final + LAG
    tokens = ids_ref.shape[1]
    dp = lax.axis_index("dp")
    me = lax.axis_index("expert")
    e, lane = me // SPLIT, me % SPLIT
    across = me - lane + (lane + 2) % SPLIT
    beside = me - lane + (lane // 2) * 2 + (lane + 1) % 2
    lane_across = (lane + 2) % SPLIT
    paired = experts & (experts - 1) == 0
    steps = sorted(range(1, experts), key=lambda k: -(k.bit_length()))

    def partner(k):
        if not paired:
            return (e + k) % experts
        there = e
        for bit in range(k.bit_length()):
            if k >> bit & 1:
                there = there + (1 << bit) - (2 << bit) * (e // (1 << bit) % 2)
        return there

    def origin(k):
        return partner(k) if paired else (e + experts - k) % experts

    def share_of(ref, share):
        if aligned:
            return ref.at[:, pl.ds(pl.multiple_of(share * own * width, 128), own * width)]
        return ref.at[pl.ds(share * own, own)]

    loads = [
        pltpu.make_async_copy(source, to, load.at[i])
        for i, (source, to) in enumerate(
            (
                (ids_hbm, ids_ref),
                (weights_hbm, weights_ref),
                (share_of(cot_hbm, dp), share_of(cot_ref, dp)),
                (gate_hbm, gate_ref),
                (up_hbm, up_ref),
                (down_hbm, down_ref),
            )
        )
    ]
    others = [
        pltpu.make_async_copy(
            share_of(cot_hbm, (dp + k) % n), share_of(cot_ref, (dp + k) % n), load.at[5 + k]
        )
        for k in range(1, n)
    ]
    for copy in loads[:3] + others:
        copy.start()

    barrier = pltpu.get_barrier_semaphore()

    def greet(target):
        pl.semaphore_signal(
            barrier, inc=1, device_id=target, device_id_type=pl.DeviceIdType.MESH
        )

    for k in steps:
        greet({"expert": partner(k) * SPLIT + lane})
    greet({"expert": across})
    greet({"expert": beside})
    for k in range(1, n):
        greet({"dp": (dp + k) % n})

    def send(source, to, sent, arrived, device):
        return pltpu.make_async_remote_copy(
            src_ref=source,
            dst_ref=to,
            send_sem=sent,
            recv_sem=arrived,
            device_id=device,
            device_id_type=pl.DeviceIdType.MESH,
        )

    def chunk_at(t):
        late = jnp.where(t < early + away, own - early, -away)
        return t + jnp.where(t < early, 0, late)

    def columns_of(share, j):
        if aligned:
            return cot_ref.at[:, pl.ds(pl.multiple_of((share * own + j) * width, 128), width)]
        return cot_ref.at[share * own + j]

    def cot_copy(i):
        to = (dp - 1 - i // own + n) % n
        return send(columns_of(to, i % own), cot_in.at[i], x_send.at[0], x_recv.at[i], {"dp": to})

    def ids_copy(k):
        return send(
            ids_ref, ids_in.at[k - 1], i_send.at[k - 1, 0], i_recv.at[k - 1, 0], {"dp": (dp - k + n) % n}
        )

    def weights_copy(k):
        return send(
            weights_ref, weights_in.at[k - 1], i_send.at[k - 1, 1], i_recv.at[k - 1, 1], {"dp": (dp - k + n) % n}
        )

    def product_copy(k):
        return send(
            product.at[0], product.at[k], p_send.at[k - 1], p_recv.at[k - 1], {"dp": (dp - k + n) % n}
        )

    def up_copy(i, plane):
        at = pl.ds(pl.multiple_of(plane * block, 16), block)
        return send(
            up_out.at[i, at], up_in.at[i, at], u_send.at[i], u_recv.at[i], {"dp": (dp + 1 + i) % n}
        )

    def pick(k, ids_row, weight_row):
        shape = (tokens, tokens)
        first = lax.broadcasted_iota(jnp.int32, shape, 0)
        second = lax.broadcasted_iota(jnp.int32, shape, 1)
        names = lax.broadcasted_iota(jnp.int32, (-(-experts // 16) * 16, tokens), 0) == ids_row
        before = jnp.where(first < second, 1.0, 0.0).astype(jnp.bfloat16)
        earlier = jnp.dot(
            jnp.where(names, 1.0, 0.0).astype(jnp.bfloat16), before, preferred_element_type=jnp.float32
        )
        position = jnp.sum(jnp.where(names, earlier, 0.0), axis=0, keepdims=True).astype(jnp.int32)
        target = ids_row * cap + position
        chosen = lax.broadcasted_iota(jnp.int32, (experts * cap, tokens), 0) == target
        picker[k] = jnp.where(chosen, 1.0, 0.0).astype(jnp.bfloat16)
        scale[k] = jnp.sum(jnp.where(chosen, weight_row, 0.0), axis=1, keepdims=True)

    def place(q, k, columns):
        picked = jnp.dot(picker[k], columns, preferred_element_type=jnp.float32)
        rows = (picked * scale[k]).astype(jnp.bfloat16).reshape(experts, cap, width)
        sendbuf[q] = rows
        routed[q, e, lane] = sendbuf[q, e]

    def build(t):
        q = chunk_at(t)

        @pl.when(q >= own)
        def _():
            cot_copy(q - own).wait_recv()
            place(q, q // own, cot_in[q - own])

    def to_across(q, plane, arrived):
        at = routed.at[q, plane, lane]
        send(at, at, y_send.at[0], arrived, {"expert": across}).start()

    def to_beside(at, arrived):
        send(at, at, c_send.at[0], arrived, {"expert": beside}).start()

    def forward_across(q):
        all_of(routed.at[q, pl.ds(0, experts - 1), 0], y_recv.at[q])
        for k in steps:
            to_beside(routed.at[q, origin(k), lane_across], c_recv.at[q])

    def to_plane(source, to, k, arrived):
        send(source, to, z_send.at[0], arrived, {"expert": partner(k) * SPLIT + lane}).start()

    def to_expert(t):
        q = chunk_at(t)
        for i, k in enumerate(steps):
            arrived = z_recv.at[t + (jnp.where(t == final, i, 0) if i else 0)]
            to_plane(sendbuf.at[q, partner(k)], routed.at[q, e, lane], k, arrived)

        @pl.when(q >= own)
        def _():
            to_across(q, e, y_recv.at[chunks + 1])

    def all_of(ref_at, sem):
        pltpu.make_async_copy(ref_at, ref_at, sem).wait()

    def forward(q, k):
        plane = origin(k)
        to_across(q, plane, y_recv.at[q])
        to_beside(routed.at[q, plane, lane], c_recv.at[q])

    loads[0].wait()
    loads[1].wait()
    pick(0, ids_ref[...], weights_ref[...])
    loads[2].wait()
    for j in range(early):
        place(j, 0, columns_of(dp, j)[...])
    pl.semaphore_wait(barrier, experts - 1 + 2 + n - 1)
    for j in range(early):
        to_expert(j)
    for k in range(1, n):
        ids_copy(k).start()
        weights_copy(k).start()
    for copy in others:
        copy.wait()

    @pl.loop(0, away)
    def _(i):
        cot_copy(i).start()

    for copy in loads[3:]:
        copy.start()
    for j in range(early):
        to_across(j, e, y_recv.at[chunks])

    @pl.loop(early, own)
    def _(j):
        place(j, 0, columns_of(dp, j)[...])

    rows_all = gate_ref.shape[0]
    piece = rows_all // 8
    loads[3].wait()
    loads[4].wait()

    @pl.loop(0, 8)
    def _(i):
        at = pl.ds(pl.multiple_of(i * piece, 16), piece)
        gate = gate_ref[at, :].astype(jnp.float32)
        up = up_ref[at, :].astype(jnp.float32)
        sig = jax.nn.sigmoid(gate)
        act = gate * sig
        active[at, :] = act
        slope[at, :] = up * sig * (1.0 + gate * (1.0 - sig))
        product[0, at, :] = (act * up).astype(jnp.bfloat16)
        for k in range(n):
            upstream[k, at, :] = jnp.zeros_like(act)

    @pl.loop(early, own)
    def _(j):
        to_across(j, e, y_recv.at[chunks])

    to_beside(routed.at[pl.ds(0, own), e, lane], c_recv.at[chunks])

    for k in range(1, n):
        ids_copy(k).wait_recv()
        weights_copy(k).wait_recv()
        pick(k, ids_in[k - 1], weights_in[k - 1])
    for t in range(early, ahead):
        build(t)
    for k in range(1, n):
        product_copy(k).start()
    loads[5].wait()
    for t in range(early, ahead):
        to_expert(t)

    def gradient(j):
        total = jnp.zeros((width, product.shape[2]), jnp.float32)
        for k in range(n):
            rows = routed[k * own + j].reshape(rows_all, width)
            total = total + lax.dot_general(
                rows, product[k], (((0,), (0,)), ((), ())), preferred_element_type=jnp.float32
            )
        wgrad_ref[j] = total.astype(jnp.bfloat16)

    def compute(turn):
        q = chunk_at(turn)
        k, j = q // own, q % own

        @pl.when(turn == 0)
        def _():
            all_of(routed.at[pl.ds(0, own), 0, pl.ds(0, 2)], c_recv.at[chunks])

        all_of(routed.at[q, pl.ds(0, experts - 1), pl.ds(0, 2)], c_recv.at[q])

        @pl.when(k == 0)
        def _():
            rows = routed[q].reshape(rows_all, width)
            upstream[0] += jnp.dot(rows, down_ref[j], preferred_element_type=jnp.float32)

        @pl.when(k >= 1)
        def _():
            for step in steps:
                plane = origin(step)
                at = pl.ds(pl.multiple_of(plane * block, 16), block)
                rows = routed[q, plane].reshape(block, width)
                upstream[k, at, :] += jnp.dot(rows, down_ref[j], preferred_element_type=jnp.float32)

                @pl.when(j == own - 1)
                def _():
                    up_out[k - 1, at, :] = upstream[k, at, :].astype(jnp.bfloat16)

        @pl.when(turn >= early + away)
        def _():
            gradient(j)

        @pl.when((k >= 1) & (j == own - 1))
        def _():
            for step in steps:
                up_copy(k - 1, origin(step)).start()

    def early_gradients():
        for k in range(1, n):
            product_copy(k).wait_recv()
        for j in range(early):
            gradient(j)

    @pl.loop(0, steady)
    def _(t):
        @pl.when(t >= LAG)
        def _():
            @pl.when(t == LAG)
            def _():
                all_of(routed.at[pl.ds(0, own), 0, 0], y_recv.at[chunks])
                to_beside(routed.at[pl.ds(0, own), e, lane_across], c_recv.at[chunks])

            forward_across(chunk_at(t - LAG))

        @pl.when(t < final)
        def _():
            q = chunk_at(t)
            all_of(routed.at[q, pl.ds(0, experts - 1), 0], z_recv.at[t])
            for k in steps:
                forward(q, k)

        @pl.when(t == final)
        def _():
            for i, k in enumerate(steps):
                all_of(routed.at[own - 1, 0, 0], z_recv.at[final + i])
                forward(own - 1, k)

        @pl.when(t + ahead < early + away)
        def _():
            build(t + ahead)

        @pl.when(t == home_turn)
        def _():
            theirs = pl.ds(own, away)
            to_beside(routed.at[theirs, e, lane], c_recv.at[chunks + 1])
            all_of(routed.at[theirs, 0, 0], y_recv.at[chunks + 1])
            to_beside(routed.at[theirs, e, lane_across], c_recv.at[chunks + 1])

        @pl.when(t == home_turn + 1)
        def _():
            all_of(routed.at[pl.ds(own, away), 0, pl.ds(0, 2)], c_recv.at[chunks + 1])
            at = pl.ds(pl.multiple_of(e * block, 16), block)
            for k in range(1, n):
                total = jnp.zeros((block, product.shape[2]), jnp.float32)
                for j in range(own):
                    rows = routed[k * own + j, e].reshape(block, width)
                    total = total + jnp.dot(rows, down_ref[j], preferred_element_type=jnp.float32)
                up_out[k - 1, at, :] = total.astype(jnp.bfloat16)

        @pl.when(t == rush + 1)
        def _():
            early_gradients()

        @pl.loop(t - LAG - 1 + jnp.where(t == rush + 1, 1, 0), t - LAG + jnp.where(t == rush, 1, 0))
        def _(turn):
            @pl.when(turn >= 0)
            def _():
                compute(turn)

        @pl.when(t == home_turn + 1)
        def _():
            for k in range(1, n):
                up_copy(k - 1, e).start()

        @pl.when(t + ahead < chunks)
        def _():
            to_expert(t + ahead)

    forward_across(own - 1)
    if rush + 1 >= steady:
        early_gradients()

    @pl.loop(final if rush == steady - 1 else final - 1, chunks)
    def _(turn):
        compute(turn)

    for k in range(1, n):
        all_of(up_in.at[k - 1], u_recv.at[k - 1])

    @pl.loop(0, 8)
    def _(i):
        at = pl.ds(pl.multiple_of(i * piece, 16), piece)
        total = upstream[0, at, :]
        for k in range(1, n):
            total = total + up_in[k - 1, at, :].astype(jnp.float32)
        ggrad_ref[at, :] = (total * slope[at, :]).astype(jnp.bfloat16)
        ugrad_ref[at, :] = (total * active[at, :]).astype(jnp.bfloat16)

    all_of(sendbuf.at[:, pl.ds(0, experts - 1)], z_send.at[0])
    all_of(sendbuf, y_send.at[0])
    all_of(routed.at[:, :, pl.ds(0, 2)], c_send.at[0])
    all_of(cot_in, x_send.at[0])
    for k in range(1, n):
        ids_copy(k).wait_send()
        weights_copy(k).wait_send()
        product_copy(k).wait_send()
        all_of(up_out.at[k - 1], u_send.at[k - 1])


def store(*refs):
    count = len(refs) // 2
    copies = [pltpu.make_async_copy(refs[i], refs[count + i], refs[-1].at[i]) for i in range(count)]
    for copy in copies:
        copy.start()
    for copy in copies:
        copy.wait()


def chunk_width(depth):
    for width in (256, 128):
        if depth % width == 0:
            return width, True
    return depth, False


def per_device(cotangent, expert_ids, route_weights, gate_pre, up_pre, down_weight):
    n = lax.axis_size("dp")
    devices = lax.axis_size("expert")
    experts = devices // SPLIT
    rows, hidden = gate_pre.shape
    capacity = rows // devices
    cap = -(-capacity // 16) * 16
    depth = down_weight.shape[0]
    width, aligned = chunk_width(depth)
    own = depth // width
    chunks = n * own
    away = chunks - own
    if not aligned:
        cotangent = cotangent.reshape(-1, chunks, width).swapaxes(0, 1)

    def widen(a):
        if cap == capacity:
            return a
        a = a.reshape(devices, capacity, hidden)
        return jnp.pad(a, ((0, 0), (0, cap - capacity), (0, 0))).reshape(devices * cap, hidden)

    def narrow(a):
        if cap == capacity:
            return a
        return a.reshape(devices, cap, hidden)[:, :capacity].reshape(rows, hidden)

    padded = devices * cap
    tokens = expert_ids.shape[0]
    half, full = jnp.bfloat16, jnp.float32
    vmem = pl.BlockSpec(memory_space=pltpu.VMEM)
    anywhere = pl.BlockSpec(memory_space=pltpu.HBM)
    dma = pltpu.SemaphoreType.DMA
    weight_grad, gate_grad, up_grad = pl.pallas_call(
        functools.partial(kernel, (n, experts, cap, chunks, width, aligned)),
        out_shape=(
            pltpu.VMEM((own, width, hidden), half),
            pltpu.VMEM((padded, hidden), half),
            pltpu.VMEM((padded, hidden), half),
        ),
        in_specs=[anywhere] * 6,
        out_specs=(vmem, vmem, vmem),
        scratch_shapes=[
            pltpu.VMEM(cotangent.shape, half),
            pltpu.VMEM((1, tokens), jnp.int32),
            pltpu.VMEM((1, tokens), full),
            pltpu.VMEM((padded, hidden), half),
            pltpu.VMEM((padded, hidden), half),
            pltpu.VMEM((own, width, hidden), half),
            dma((5 + n,)),
            pltpu.VMEM((chunks, experts, cap, width), half),
            pltpu.VMEM((chunks, experts, SPLIT, cap, width), half),
            pltpu.VMEM((away, tokens, width), half),
            pltpu.VMEM((n - 1, 1, tokens), jnp.int32),
            pltpu.VMEM((n - 1, 1, tokens), full),
            pltpu.VMEM((n - 1, padded, hidden), half),
            pltpu.VMEM((n - 1, padded, hidden), half),
            pltpu.VMEM((n, padded, hidden), full),
            pltpu.VMEM((padded, hidden), full),
            pltpu.VMEM((padded, hidden), full),
            pltpu.VMEM((n, padded, hidden), half),
            pltpu.VMEM((n, experts * cap, tokens), half),
            pltpu.VMEM((n, experts * cap, 1), full),
            dma((1,)),
            dma((chunks + experts - 2,)),
            dma((1,)),
            dma((chunks + 2,)),
            dma((1,)),
            dma((chunks + 2,)),
            dma((1,)),
            dma((away,)),
            dma((n - 1, 2)),
            dma((n - 1, 2)),
            dma((n - 1,)),
            dma((n - 1,)),
            dma((n - 1,)),
            dma((n - 1,)),
        ],
        compiler_params=pltpu.CompilerParams(collective_id=0, has_side_effects=True),
    )(
        cotangent,
        expert_ids.reshape(1, -1),
        route_weights.reshape(1, -1),
        widen(gate_pre),
        widen(up_pre),
        down_weight.reshape(own, width, hidden),
    )
    results = (weight_grad.reshape(depth, hidden), gate_grad, up_grad)
    weight_grad, gate_grad, up_grad = pl.pallas_call(
        store,
        out_shape=[jax.ShapeDtypeStruct(a.shape, a.dtype) for a in results],
        in_specs=[vmem] * len(results),
        out_specs=[anywhere] * len(results),
        scratch_shapes=[dma((len(results),))],
        compiler_params=pltpu.CompilerParams(vmem_limit_bytes=1 << 22),
    )(*results)
    return weight_grad, narrow(gate_grad), narrow(up_grad)


def solution(mesh):
    placed = (
        P(("dp", "expert"), None),
        P(("dp", "expert"), None),
        P(("dp", "expert"), None),
        P("dp", "expert"),
        P("dp", "expert"),
        P("dp", "expert"),
    )
    return jax.shard_map(
        per_device,
        mesh=mesh,
        in_specs=placed,
        out_specs=(P("dp", "expert"), P("dp", "expert"), P("dp", "expert")),
        check_vma=False,
    )
```

```python
import functools
import math

import jax
import jax.numpy as jnp
from jax import lax
from jax.experimental import pallas as pl
from jax.experimental.pallas import tpu as pltpu
from jax.sharding import PartitionSpec as P

SPLIT = 4
EARLY = 2
BUILD = 3
LAG = 2
VMEM_BYTES = 66400000
LAST_LIMIT = 12 << 20


def kernel(
    sizes,
    cot_hbm,
    ids_hbm,
    weights_hbm,
    gate_hbm,
    up_hbm,
    down_hbm,
    wgrad_ref,
    routed,
    product,
    upstream,
    up_in,
    slope,
    active,
    spare,
    cot_ref,
    ids_ref,
    weights_ref,
    gate_ref,
    up_ref,
    down_ref,
    load,
    sendbuf,
    cot_in,
    ids_in,
    weights_in,
    up_out,
    picker,
    scale,
    z_send,
    z_recv,
    y_send,
    y_recv,
    c_send,
    c_recv,
    x_send,
    x_recv,
    i_send,
    i_recv,
    p_send,
    p_recv,
    u_send,
    u_recv,
):
    n, experts, cap, chunks, width, aligned = sizes
    own = chunks // n
    away = chunks - own
    early = min(EARLY, own - 1)
    ahead = min(BUILD, chunks)
    home_turn = max(0, early + away - ahead) + 1
    block = SPLIT * cap
    final = chunks - 1
    rush = early + away + 1
    steady = final + LAG
    tokens = ids_ref.shape[1]
    dp = lax.axis_index("dp")
    me = lax.axis_index("expert")
    e, lane = me // SPLIT, me % SPLIT
    across = me - lane + (lane + 2) % SPLIT
    beside = me - lane + (lane // 2) * 2 + (lane + 1) % 2
    lane_across = (lane + 2) % SPLIT
    paired = experts & (experts - 1) == 0
    steps = sorted(range(1, experts), key=lambda k: -(k.bit_length()))

    def partner(k):
        if not paired:
            return (e + k) % experts
        there = e
        for bit in range(k.bit_length()):
            if k >> bit & 1:
                there = there + (1 << bit) - (2 << bit) * (e // (1 << bit) % 2)
        return there

    def origin(k):
        return partner(k) if paired else (e + experts - k) % experts

    def share_of(ref, share):
        if aligned:
            return ref.at[:, pl.ds(pl.multiple_of(share * own * width, 128), own * width)]
        return ref.at[pl.ds(share * own, own)]

    loads = [
        pltpu.make_async_copy(source, to, load.at[i])
        for i, (source, to) in enumerate(
            (
                (ids_hbm, ids_ref),
                (weights_hbm, weights_ref),
                (share_of(cot_hbm, dp), share_of(cot_ref, dp)),
                (gate_hbm, gate_ref),
                (up_hbm, up_ref),
                (down_hbm, down_ref),
            )
        )
    ]
    others = [
        pltpu.make_async_copy(
            share_of(cot_hbm, (dp + k) % n), share_of(cot_ref, (dp + k) % n), load.at[5 + k]
        )
        for k in range(1, n)
    ]
    for copy in loads[:3] + others:
        copy.start()

    barrier = pltpu.get_barrier_semaphore()

    def greet(target):
        pl.semaphore_signal(
            barrier, inc=1, device_id=target, device_id_type=pl.DeviceIdType.MESH
        )

    for k in steps:
        greet({"expert": partner(k) * SPLIT + lane})
    greet({"expert": across})
    greet({"expert": beside})
    for k in range(1, n):
        greet({"dp": (dp + k) % n})

    def send(source, to, sent, arrived, device):
        return pltpu.make_async_remote_copy(
            src_ref=source,
            dst_ref=to,
            send_sem=sent,
            recv_sem=arrived,
            device_id=device,
            device_id_type=pl.DeviceIdType.MESH,
        )

    def chunk_at(t):
        late = jnp.where(t < early + away, own - early, -away)
        return t + jnp.where(t < early, 0, late)

    def columns_of(share, j):
        if aligned:
            return cot_ref.at[:, pl.ds(pl.multiple_of((share * own + j) * width, 128), width)]
        return cot_ref.at[share * own + j]

    def cot_copy(i):
        to = (dp - 1 - i // own + n) % n
        return send(columns_of(to, i % own), cot_in.at[i], x_send.at[0], x_recv.at[i], {"dp": to})

    def ids_copy(k):
        return send(
            ids_ref, ids_in.at[k - 1], i_send.at[k - 1, 0], i_recv.at[k - 1, 0], {"dp": (dp - k + n) % n}
        )

    def weights_copy(k):
        return send(
            weights_ref, weights_in.at[k - 1], i_send.at[k - 1, 1], i_recv.at[k - 1, 1], {"dp": (dp - k + n) % n}
        )

    def product_copy(k):
        return send(
            product.at[0], product.at[k], p_send.at[k - 1], p_recv.at[k - 1], {"dp": (dp - k + n) % n}
        )

    def up_copy(i, plane):
        at = pl.ds(pl.multiple_of(plane * block, 16), block)
        return send(
            up_out.at[i, at], up_in.at[i, at], u_send.at[i], u_recv.at[i], {"dp": (dp + 1 + i) % n}
        )

    def pick(k, ids_row, weight_row):
        shape = (tokens, tokens)
        first = lax.broadcasted_iota(jnp.int32, shape, 0)
        second = lax.broadcasted_iota(jnp.int32, shape, 1)
        names = lax.broadcasted_iota(jnp.int32, (-(-experts // 16) * 16, tokens), 0) == ids_row
        before = jnp.where(first < second, 1.0, 0.0).astype(jnp.bfloat16)
        earlier = jnp.dot(
            jnp.where(names, 1.0, 0.0).astype(jnp.bfloat16), before, preferred_element_type=jnp.float32
        )
        position = jnp.sum(jnp.where(names, earlier, 0.0), axis=0, keepdims=True).astype(jnp.int32)
        target = ids_row * cap + position
        chosen = lax.broadcasted_iota(jnp.int32, (experts * cap, tokens), 0) == target
        picker[k] = jnp.where(chosen, 1.0, 0.0).astype(jnp.bfloat16)
        scale[k] = jnp.sum(jnp.where(chosen, weight_row, 0.0), axis=1, keepdims=True)

    def place(q, k, columns):
        picked = jnp.dot(picker[k], columns, preferred_element_type=jnp.float32)
        rows = (picked * scale[k]).astype(jnp.bfloat16).reshape(experts, cap, width)
        sendbuf[q] = rows
        routed[q, e, lane] = sendbuf[q, e]

    def build(t):
        q = chunk_at(t)

        @pl.when(q >= own)
        def _():
            cot_copy(q - own).wait_recv()
            place(q, q // own, cot_in[q - own])

    def to_across(q, plane, arrived):
        at = routed.at[q, plane, lane]
        send(at, at, y_send.at[0], arrived, {"expert": across}).start()

    def to_beside(at, arrived):
        send(at, at, c_send.at[0], arrived, {"expert": beside}).start()

    def forward_across(q):
        all_of(routed.at[q, pl.ds(0, experts - 1), 0], y_recv.at[q])
        for k in steps:
            to_beside(routed.at[q, origin(k), lane_across], c_recv.at[q])

    def to_plane(source, to, k, arrived):
        send(source, to, z_send.at[0], arrived, {"expert": partner(k) * SPLIT + lane}).start()

    def to_expert(t):
        q = chunk_at(t)
        for i, k in enumerate(steps):
            arrived = z_recv.at[t + (jnp.where(t == final, i, 0) if i else 0)]
            to_plane(sendbuf.at[q, partner(k)], routed.at[q, e, lane], k, arrived)

        @pl.when(q >= own)
        def _():
            to_across(q, e, y_recv.at[chunks + 1])

    def all_of(ref_at, sem):
        pltpu.make_async_copy(ref_at, ref_at, sem).wait()

    def forward(q, k):
        plane = origin(k)
        to_across(q, plane, y_recv.at[q])
        to_beside(routed.at[q, plane, lane], c_recv.at[q])

    loads[0].wait()
    loads[1].wait()
    pick(0, ids_ref[...], weights_ref[...])
    loads[2].wait()
    for j in range(early):
        place(j, 0, columns_of(dp, j)[...])
    pl.semaphore_wait(barrier, experts - 1 + 2 + n - 1)
    for j in range(early):
        to_expert(j)
    for k in range(1, n):
        ids_copy(k).start()
        weights_copy(k).start()
    for copy in others:
        copy.wait()

    @pl.loop(0, away)
    def _(i):
        cot_copy(i).start()

    for copy in loads[3:]:
        copy.start()
    for j in range(early):
        to_across(j, e, y_recv.at[chunks])

    @pl.loop(early, own)
    def _(j):
        place(j, 0, columns_of(dp, j)[...])

    rows_all = gate_ref.shape[0]
    piece = rows_all // 8
    loads[3].wait()
    loads[4].wait()

    @pl.loop(0, 8)
    def _(i):
        at = pl.ds(pl.multiple_of(i * piece, 16), piece)
        gate = gate_ref[at, :].astype(jnp.float32)
        up = up_ref[at, :].astype(jnp.float32)
        sig = jax.nn.sigmoid(gate)
        act = gate * sig
        active[at, :] = act
        slope[at, :] = up * sig * (1.0 + gate * (1.0 - sig))
        product[0, at, :] = (act * up).astype(jnp.bfloat16)
        for k in range(n):
            upstream[k, at, :] = jnp.zeros_like(act)

    @pl.loop(early, own)
    def _(j):
        to_across(j, e, y_recv.at[chunks])

    to_beside(routed.at[pl.ds(0, own), e, lane], c_recv.at[chunks])

    for k in range(1, n):
        ids_copy(k).wait_recv()
        weights_copy(k).wait_recv()
        pick(k, ids_in[k - 1], weights_in[k - 1])
    for t in range(early, ahead):
        build(t)
    for k in range(1, n):
        product_copy(k).start()
    loads[5].wait()
    for t in range(early, ahead):
        to_expert(t)

    def gradient(j):
        total = jnp.zeros((width, product.shape[2]), jnp.float32)
        wgrad_ref[j] = down_gradient(routed, product, own, j, range(n), total).astype(jnp.bfloat16)

    def compute(turn):
        q = chunk_at(turn)
        k, j = q // own, q % own

        @pl.when(turn == 0)
        def _():
            all_of(routed.at[pl.ds(0, own), 0, pl.ds(0, 2)], c_recv.at[chunks])

        all_of(routed.at[q, pl.ds(0, experts - 1), pl.ds(0, 2)], c_recv.at[q])

        @pl.when(k == 0)
        def _():
            rows = routed[q].reshape(rows_all, width)
            upstream[0] += jnp.dot(rows, down_ref[j], preferred_element_type=jnp.float32)

        @pl.when(k >= 1)
        def _():
            for step in steps:
                plane = origin(step)
                at = pl.ds(pl.multiple_of(plane * block, 16), block)
                rows = routed[q, plane].reshape(block, width)
                upstream[k, at, :] += jnp.dot(rows, down_ref[j], preferred_element_type=jnp.float32)

                @pl.when(j == own - 1)
                def _():
                    up_out[k - 1, at, :] = upstream[k, at, :].astype(jnp.bfloat16)

        @pl.when((turn >= early + away) & (turn < final))
        def _():
            gradient(j)

        @pl.when((k >= 1) & (j == own - 1))
        def _():
            for step in steps:
                up_copy(k - 1, origin(step)).start()

    def early_gradients():
        for k in range(1, n):
            product_copy(k).wait_recv()
        for j in range(early):
            gradient(j)
        total = jnp.zeros((width, product.shape[2]), jnp.float32)
        spare[...] = down_gradient(routed, product, own, own - 1, range(1, n), total)

    @pl.loop(0, steady)
    def _(t):
        @pl.when(t >= LAG)
        def _():
            @pl.when(t == LAG)
            def _():
                all_of(routed.at[pl.ds(0, own), 0, 0], y_recv.at[chunks])
                to_beside(routed.at[pl.ds(0, own), e, lane_across], c_recv.at[chunks])

            forward_across(chunk_at(t - LAG))

        @pl.when(t < final)
        def _():
            q = chunk_at(t)
            all_of(routed.at[q, pl.ds(0, experts - 1), 0], z_recv.at[t])
            for k in steps:
                forward(q, k)

        @pl.when(t == final)
        def _():
            for i, k in enumerate(steps):
                all_of(routed.at[own - 1, 0, 0], z_recv.at[final + i])
                forward(own - 1, k)

        @pl.when(t + ahead < early + away)
        def _():
            build(t + ahead)

        @pl.when(t == home_turn)
        def _():
            theirs = pl.ds(own, away)
            to_beside(routed.at[theirs, e, lane], c_recv.at[chunks + 1])
            all_of(routed.at[theirs, 0, 0], y_recv.at[chunks + 1])
            to_beside(routed.at[theirs, e, lane_across], c_recv.at[chunks + 1])

        @pl.when(t == home_turn + 1)
        def _():
            all_of(routed.at[pl.ds(own, away), 0, pl.ds(0, 2)], c_recv.at[chunks + 1])
            at = pl.ds(pl.multiple_of(e * block, 16), block)
            for k in range(1, n):
                total = jnp.zeros((block, product.shape[2]), jnp.float32)
                for j in range(own):
                    rows = routed[k * own + j, e].reshape(block, width)
                    total = total + jnp.dot(rows, down_ref[j], preferred_element_type=jnp.float32)
                up_out[k - 1, at, :] = total.astype(jnp.bfloat16)

        @pl.when(t == rush + 1)
        def _():
            early_gradients()

        @pl.loop(t - LAG - 1 + jnp.where(t == rush + 1, 1, 0), t - LAG + jnp.where(t == rush, 1, 0))
        def _(turn):
            @pl.when(turn >= 0)
            def _():
                compute(turn)

        @pl.when(t == home_turn + 1)
        def _():
            for k in range(1, n):
                up_copy(k - 1, e).start()

        @pl.when(t + ahead < chunks)
        def _():
            to_expert(t + ahead)

    forward_across(own - 1)
    if rush + 1 >= steady:
        early_gradients()

    @pl.loop(final if rush == steady - 1 else final - 1, chunks)
    def _(turn):
        compute(turn)

    for k in range(1, n):
        all_of(up_in.at[k - 1], u_recv.at[k - 1])

    all_of(sendbuf.at[:, pl.ds(0, experts - 1)], z_send.at[0])
    all_of(sendbuf, y_send.at[0])
    all_of(routed.at[:, :, pl.ds(0, 2)], c_send.at[0])
    all_of(cot_in, x_send.at[0])
    for k in range(1, n):
        ids_copy(k).wait_send()
        weights_copy(k).wait_send()
        product_copy(k).wait_send()
        all_of(up_out.at[k - 1], u_send.at[k - 1])


def down_gradient(routed, product, own, j, shares, total):
    rows_all = product.shape[1]
    width = routed.shape[-1]
    for k in shares:
        rows = routed[k * own + j].reshape(rows_all, width)
        total = total + lax.dot_general(
            rows, product[k], (((0,), (0,)), ((), ())), preferred_element_type=jnp.float32
        )
    return total


def finish(
    wgrad_ref,
    routed,
    product,
    upstream,
    up_in,
    slope,
    active,
    spare,
    wgrad_out,
    ggrad_out,
    ugrad_out,
    wgrad_last,
    ggrad_ref,
    ugrad_ref,
    stored,
):
    own = wgrad_ref.shape[0]
    n, rows_all, _ = product.shape
    piece = rows_all // 8
    copies = [
        pltpu.make_async_copy(source, to, stored.at[i])
        for i, (source, to) in enumerate(
            (
                (ggrad_ref, ggrad_out),
                (ugrad_ref, ugrad_out),
                (wgrad_last, wgrad_out.at[own - 1]),
            )
        )
    ]
    if own > 1:
        done = pl.ds(0, own - 1)
        copies.append(pltpu.make_async_copy(wgrad_ref.at[done], wgrad_out.at[done], stored.at[3]))
        copies[3].start()

    @pl.loop(0, 8)
    def _(i):
        at = pl.ds(pl.multiple_of(i * piece, 16), piece)
        total = upstream[0, at, :]
        for k in range(1, n):
            total = total + up_in[k - 1, at, :].astype(jnp.float32)
        ggrad_ref[at, :] = (total * slope[at, :]).astype(jnp.bfloat16)
        ugrad_ref[at, :] = (total * active[at, :]).astype(jnp.bfloat16)

    copies[0].start()
    copies[1].start()
    wgrad_last[...] = down_gradient(routed, product, own, own - 1, range(1), spare[...]).astype(jnp.bfloat16)
    copies[2].start()
    for copy in copies:
        copy.wait()


def chunk_width(depth):
    for width in (256, 128):
        if depth % width == 0:
            return width, True
    return depth, False


def per_device(cotangent, expert_ids, route_weights, gate_pre, up_pre, down_weight):
    n = lax.axis_size("dp")
    devices = lax.axis_size("expert")
    experts = devices // SPLIT
    rows, hidden = gate_pre.shape
    capacity = rows // devices
    cap = -(-capacity // 16) * 16
    depth = down_weight.shape[0]
    width, aligned = chunk_width(depth)
    own = depth // width
    chunks = n * own
    away = chunks - own
    if not aligned:
        cotangent = cotangent.reshape(-1, chunks, width).swapaxes(0, 1)

    def widen(a):
        if cap == capacity:
            return a
        a = a.reshape(devices, capacity, hidden)
        return jnp.pad(a, ((0, 0), (0, cap - capacity), (0, 0))).reshape(devices * cap, hidden)

    def narrow(a):
        if cap == capacity:
            return a
        return a.reshape(devices, cap, hidden)[:, :capacity].reshape(rows, hidden)

    padded = devices * cap
    tokens = expert_ids.shape[0]
    half, full = jnp.bfloat16, jnp.float32
    vmem = pl.BlockSpec(memory_space=pltpu.VMEM)
    anywhere = pl.BlockSpec(memory_space=pltpu.HBM)
    dma = pltpu.SemaphoreType.DMA
    kept = (
        pltpu.VMEM((own, width, hidden), half),
        pltpu.VMEM((chunks, experts, SPLIT, cap, width), half),
        pltpu.VMEM((n, padded, hidden), half),
        pltpu.VMEM((n, padded, hidden), full),
        pltpu.VMEM((n - 1, padded, hidden), half),
        pltpu.VMEM((padded, hidden), full),
        pltpu.VMEM((padded, hidden), full),
        pltpu.VMEM((width, hidden), full),
    )
    held = sum(
        math.prod(a.shape[:-1]) * -(-a.shape[-1] // 128) * 128 * jnp.dtype(a.dtype).itemsize for a in kept
    )
    parts = pl.pallas_call(
        functools.partial(kernel, (n, experts, cap, chunks, width, aligned)),
        out_shape=kept,
        in_specs=[anywhere] * 6,
        out_specs=(vmem,) * len(kept),
        scratch_shapes=[
            pltpu.VMEM(cotangent.shape, half),
            pltpu.VMEM((1, tokens), jnp.int32),
            pltpu.VMEM((1, tokens), full),
            pltpu.VMEM((padded, hidden), half),
            pltpu.VMEM((padded, hidden), half),
            pltpu.VMEM((own, width, hidden), half),
            dma((5 + n,)),
            pltpu.VMEM((chunks, experts, cap, width), half),
            pltpu.VMEM((away, tokens, width), half),
            pltpu.VMEM((n - 1, 1, tokens), jnp.int32),
            pltpu.VMEM((n - 1, 1, tokens), full),
            pltpu.VMEM((n - 1, padded, hidden), half),
            pltpu.VMEM((n, experts * cap, tokens), half),
            pltpu.VMEM((n, experts * cap, 1), full),
            dma((1,)),
            dma((chunks + experts - 2,)),
            dma((1,)),
            dma((chunks + 2,)),
            dma((1,)),
            dma((chunks + 2,)),
            dma((1,)),
            dma((away,)),
            dma((n - 1, 2)),
            dma((n - 1, 2)),
            dma((n - 1,)),
            dma((n - 1,)),
            dma((n - 1,)),
            dma((n - 1,)),
        ],
        compiler_params=pltpu.CompilerParams(
            collective_id=0, has_side_effects=True, vmem_limit_bytes=VMEM_BYTES - held
        ),
    )(
        cotangent,
        expert_ids.reshape(1, -1),
        route_weights.reshape(1, -1),
        widen(gate_pre),
        widen(up_pre),
        down_weight.reshape(own, width, hidden),
    )
    weight_grad, gate_grad, up_grad = pl.pallas_call(
        finish,
        out_shape=(
            jax.ShapeDtypeStruct((own, width, hidden), half),
            jax.ShapeDtypeStruct((padded, hidden), half),
            jax.ShapeDtypeStruct((padded, hidden), half),
        ),
        in_specs=[vmem] * len(kept),
        out_specs=[anywhere] * 3,
        scratch_shapes=[
            pltpu.VMEM((width, hidden), half),
            pltpu.VMEM((padded, hidden), half),
            pltpu.VMEM((padded, hidden), half),
            dma((4,)),
        ],
        compiler_params=pltpu.CompilerParams(vmem_limit_bytes=LAST_LIMIT),
    )(*parts)
    weight_grad = weight_grad.reshape(depth, hidden)
    return weight_grad, narrow(gate_grad), narrow(up_grad)


def solution(mesh):
    placed = (
        P(("dp", "expert"), None),
        P(("dp", "expert"), None),
        P(("dp", "expert"), None),
        P("dp", "expert"),
        P("dp", "expert"),
        P("dp", "expert"),
    )
    return jax.shard_map(
        per_device,
        mesh=mesh,
        in_specs=placed,
        out_specs=(P("dp", "expert"), P("dp", "expert"), P("dp", "expert")),
        check_vma=False,
    )
```

```python
import functools
import math

import jax
import jax.numpy as jnp
from jax import lax
from jax.experimental import pallas as pl
from jax.experimental.pallas import tpu as pltpu
from jax.sharding import PartitionSpec as P

SPLIT = 4
EARLY = 2
BUILD = 3
LAG = 2
RING = 7
VMEM_BYTES = 66400000
LAST_LIMIT = 12 << 20


def kernel(
    sizes,
    cot_hbm,
    ids_hbm,
    weights_hbm,
    gate_hbm,
    up_hbm,
    down_hbm,
    wgrad_ref,
    routed,
    product,
    upstream,
    up_in,
    slope,
    active,
    spare,
    cot_ref,
    ids_ref,
    weights_ref,
    gate_ref,
    up_ref,
    down_ref,
    load,
    sendbuf,
    cot_in,
    ids_in,
    weights_in,
    up_out,
    picker,
    scale,
    z_send,
    z_recv,
    y_send,
    y_recv,
    c_send,
    c_recv,
    x_send,
    x_recv,
    i_send,
    i_recv,
    p_send,
    p_recv,
    u_send,
    u_recv,
):
    n, experts, cap, chunks, width, aligned = sizes
    own = chunks // n
    away = chunks - own
    early = min(EARLY, own - 1)
    ahead = min(BUILD, chunks)
    home_turn = max(0, early + away - ahead) + 1
    block = SPLIT * cap
    final = chunks - 1
    rush = early + away + 1
    steady = final + LAG
    tokens = ids_ref.shape[1]
    dp = lax.axis_index("dp")
    me = lax.axis_index("expert")
    e, lane = me // SPLIT, me % SPLIT
    across = me - lane + (lane + 2) % SPLIT
    beside = me - lane + (lane // 2) * 2 + (lane + 1) % 2
    lane_across = (lane + 2) % SPLIT
    paired = experts & (experts - 1) == 0
    steps = sorted(range(1, experts), key=lambda k: -(k.bit_length()))
    ring = min(RING, chunks)

    def partner(k):
        if not paired:
            return (e + k) % experts
        there = e
        for bit in range(k.bit_length()):
            if k >> bit & 1:
                there = there + (1 << bit) - (2 << bit) * (e // (1 << bit) % 2)
        return there

    def origin(k):
        return partner(k) if paired else (e + experts - k) % experts

    def share_of(ref, share):
        if aligned:
            return ref.at[:, pl.ds(pl.multiple_of(share * own * width, 128), own * width)]
        return ref.at[pl.ds(share * own, own)]

    loads = [
        pltpu.make_async_copy(source, to, load.at[i])
        for i, (source, to) in enumerate(
            (
                (ids_hbm, ids_ref),
                (weights_hbm, weights_ref),
                (share_of(cot_hbm, dp), share_of(cot_ref, dp)),
                (gate_hbm, gate_ref),
                (up_hbm, up_ref),
                (down_hbm, down_ref),
            )
        )
    ]
    others = [
        pltpu.make_async_copy(
            share_of(cot_hbm, (dp + k) % n), share_of(cot_ref, (dp + k) % n), load.at[5 + k]
        )
        for k in range(1, n)
    ]
    for copy in loads[:3] + others:
        copy.start()

    barrier = pltpu.get_barrier_semaphore()

    def greet(target):
        pl.semaphore_signal(
            barrier, inc=1, device_id=target, device_id_type=pl.DeviceIdType.MESH
        )

    for k in steps:
        greet({"expert": partner(k) * SPLIT + lane})
    greet({"expert": across})
    greet({"expert": beside})
    for k in range(1, n):
        greet({"dp": (dp + k) % n})

    def send(source, to, sent, arrived, device):
        return pltpu.make_async_remote_copy(
            src_ref=source,
            dst_ref=to,
            send_sem=sent,
            recv_sem=arrived,
            device_id=device,
            device_id_type=pl.DeviceIdType.MESH,
        )

    def chunk_at(t):
        late = jnp.where(t < early + away, own - early, -away)
        return t + jnp.where(t < early, 0, late)

    def columns_of(share, j):
        if aligned:
            return cot_ref.at[:, pl.ds(pl.multiple_of((share * own + j) * width, 128), width)]
        return cot_ref.at[share * own + j]

    def cot_copy(i):
        to = (dp - 1 - i // own + n) % n
        return send(columns_of(to, i % own), cot_in.at[i], x_send.at[0], x_recv.at[i], {"dp": to})

    def ids_copy(k):
        return send(
            ids_ref, ids_in.at[k - 1], i_send.at[k - 1, 0], i_recv.at[k - 1, 0], {"dp": (dp - k + n) % n}
        )

    def weights_copy(k):
        return send(
            weights_ref, weights_in.at[k - 1], i_send.at[k - 1, 1], i_recv.at[k - 1, 1], {"dp": (dp - k + n) % n}
        )

    def product_copy(k):
        return send(
            product.at[0], product.at[k], p_send.at[k - 1], p_recv.at[k - 1], {"dp": (dp - k + n) % n}
        )

    def up_copy(i, plane):
        at = pl.ds(pl.multiple_of(plane * block, 16), block)
        return send(
            up_out.at[i, at], up_in.at[i, at], u_send.at[i], u_recv.at[i], {"dp": (dp + 1 + i) % n}
        )

    def pick(k, ids_row, weight_row):
        shape = (tokens, tokens)
        first = lax.broadcasted_iota(jnp.int32, shape, 0)
        second = lax.broadcasted_iota(jnp.int32, shape, 1)
        names = lax.broadcasted_iota(jnp.int32, (-(-experts // 16) * 16, tokens), 0) == ids_row
        before = jnp.where(first < second, 1.0, 0.0).astype(jnp.bfloat16)
        earlier = jnp.dot(
            jnp.where(names, 1.0, 0.0).astype(jnp.bfloat16), before, preferred_element_type=jnp.float32
        )
        position = jnp.sum(jnp.where(names, earlier, 0.0), axis=0, keepdims=True).astype(jnp.int32)
        target = ids_row * cap + position
        chosen = lax.broadcasted_iota(jnp.int32, (experts * cap, tokens), 0) == target
        picker[k] = jnp.where(chosen, 1.0, 0.0).astype(jnp.bfloat16)
        scale[k] = jnp.sum(jnp.where(chosen, weight_row, 0.0), axis=1, keepdims=True)

    def place(q, k, columns):
        picked = jnp.dot(picker[k], columns, preferred_element_type=jnp.float32)
        rows = (picked * scale[k]).astype(jnp.bfloat16).reshape(experts, cap, width)
        sendbuf[q] = rows
        routed[q, e, lane] = sendbuf[q, e]

    def build(t):
        q = chunk_at(t)

        @pl.when(q >= own)
        def _():
            cot_copy(q - own).wait_recv()
            place(q, q // own, cot_in[q - own])

    def to_across(q, plane, arrived):
        at = routed.at[q, plane, lane]
        send(at, at, y_send.at[0], arrived, {"expert": across}).start()

    def to_beside(at, arrived):
        send(at, at, c_send.at[0], arrived, {"expert": beside}).start()

    def forward_across(t):
        q = chunk_at(t)
        all_of(routed.at[q, pl.ds(0, experts - 1), 0], y_recv.at[t % ring])
        for k in steps:
            to_beside(routed.at[q, origin(k), lane_across], c_recv.at[t % ring])

    def to_plane(source, to, there, arrived):
        send(source, to, z_send.at[0], arrived, {"expert": there * SPLIT + lane}).start()

    def z_arrived(t, i):
        return z_recv.at[jnp.where(t == final, ring + i - 1, t % ring)] if i else z_recv.at[t % ring]

    def to_expert(t):
        q = chunk_at(t)
        for i, k in enumerate(steps):
            there = partner(k)
            to_plane(sendbuf.at[q, there], routed.at[q, e, lane], there, z_arrived(t, i))

        @pl.when(q >= own)
        def _():
            to_across(q, e, y_recv.at[ring + 1])

    def all_of(ref_at, sem):
        pltpu.make_async_copy(ref_at, ref_at, sem).wait()

    def forward(t, k):
        q, plane = chunk_at(t), origin(k)
        to_across(q, plane, y_recv.at[t % ring])
        to_beside(routed.at[q, plane, lane], c_recv.at[t % ring])

    loads[0].wait()
    loads[1].wait()
    pick(0, ids_ref[...], weights_ref[...])
    loads[2].wait()
    for j in range(early):
        place(j, 0, columns_of(dp, j)[...])
    pl.semaphore_wait(barrier, experts - 1 + 2 + n - 1)
    for j in range(early):
        to_expert(j)
    for k in range(1, n):
        ids_copy(k).start()
        weights_copy(k).start()
    for copy in others:
        copy.wait()

    @pl.loop(0, away)
    def _(i):
        cot_copy(i).start()

    for copy in loads[3:]:
        copy.start()
    for j in range(early):
        to_across(j, e, y_recv.at[ring])

    @pl.loop(early, own)
    def _(j):
        place(j, 0, columns_of(dp, j)[...])

    rows_all = gate_ref.shape[0]
    piece = rows_all // 8
    loads[3].wait()
    loads[4].wait()

    @pl.loop(0, 8)
    def _(i):
        at = pl.ds(pl.multiple_of(i * piece, 16), piece)
        gate = gate_ref[at, :].astype(jnp.float32)
        up = up_ref[at, :].astype(jnp.float32)
        sig = jax.nn.sigmoid(gate)
        act = gate * sig
        active[at, :] = act
        slope[at, :] = up * sig * (1.0 + gate * (1.0 - sig))
        product[0, at, :] = (act * up).astype(jnp.bfloat16)
        for k in range(n):
            upstream[k, at, :] = jnp.zeros_like(act)

    @pl.loop(early, own)
    def _(j):
        to_across(j, e, y_recv.at[ring])

    to_beside(routed.at[pl.ds(0, own), e, lane], c_recv.at[ring])

    for k in range(1, n):
        ids_copy(k).wait_recv()
        weights_copy(k).wait_recv()
        pick(k, ids_in[k - 1], weights_in[k - 1])
    for t in range(early, ahead):
        build(t)
    for k in range(1, n):
        product_copy(k).start()
    loads[5].wait()
    for t in range(early, ahead):
        to_expert(t)

    def gradient(j):
        total = jnp.zeros((width, product.shape[2]), jnp.float32)
        wgrad_ref[j] = down_gradient(routed, product, own, j, range(n), total).astype(jnp.bfloat16)

    def compute(turn):
        q = chunk_at(turn)
        k, j = q // own, q % own

        @pl.when(turn == 0)
        def _():
            all_of(routed.at[pl.ds(0, own), 0, pl.ds(0, 2)], c_recv.at[ring])

        all_of(routed.at[q, pl.ds(0, experts - 1), pl.ds(0, 2)], c_recv.at[turn % ring])

        @pl.when(k == 0)
        def _():
            rows = routed[q].reshape(rows_all, width)
            upstream[0] += jnp.dot(rows, down_ref[j], preferred_element_type=jnp.float32)

        @pl.when(k >= 1)
        def _():
            for step in steps:
                plane = origin(step)
                at = pl.ds(pl.multiple_of(plane * block, 16), block)
                rows = routed[q, plane].reshape(block, width)
                upstream[k, at, :] += jnp.dot(rows, down_ref[j], preferred_element_type=jnp.float32)

                @pl.when(j == own - 1)
                def _():
                    up_out[k - 1, at, :] = upstream[k, at, :].astype(jnp.bfloat16)

        @pl.when((turn >= early + away) & (turn < final))
        def _():
            gradient(j)

        @pl.when((k >= 1) & (j == own - 1))
        def _():
            for step in steps:
                up_copy(k - 1, origin(step)).start()

    def early_gradients():
        for k in range(1, n):
            product_copy(k).wait_recv()
        for j in range(early):
            gradient(j)
        total = jnp.zeros((width, product.shape[2]), jnp.float32)
        spare[...] = down_gradient(routed, product, own, own - 1, range(1, n), total)

    @pl.loop(0, steady)
    def _(t):
        @pl.when(t >= LAG)
        def _():
            @pl.when(t == LAG)
            def _():
                all_of(routed.at[pl.ds(0, own), 0, 0], y_recv.at[ring])
                to_beside(routed.at[pl.ds(0, own), e, lane_across], c_recv.at[ring])

            forward_across(t - LAG)

        @pl.when(t < final)
        def _():
            all_of(routed.at[0, pl.ds(0, experts - 1), 0], z_recv.at[t % ring])
            for k in steps:
                forward(t, k)

        @pl.when(t == final)
        def _():
            for i, k in enumerate(steps):
                all_of(routed.at[own - 1, 0, 0], z_arrived(final, i))
                forward(final, k)

        @pl.when(t + ahead < early + away)
        def _():
            build(t + ahead)

        @pl.when(t == home_turn)
        def _():
            theirs = pl.ds(own, away)
            to_beside(routed.at[theirs, e, lane], c_recv.at[ring + 1])
            all_of(routed.at[theirs, 0, 0], y_recv.at[ring + 1])
            to_beside(routed.at[theirs, e, lane_across], c_recv.at[ring + 1])

        @pl.when(t == home_turn + 1)
        def _():
            all_of(routed.at[pl.ds(own, away), 0, pl.ds(0, 2)], c_recv.at[ring + 1])
            at = pl.ds(pl.multiple_of(e * block, 16), block)
            for k in range(1, n):
                total = jnp.zeros((block, product.shape[2]), jnp.float32)
                for j in range(own):
                    rows = routed[k * own + j, e].reshape(block, width)
                    total = total + jnp.dot(rows, down_ref[j], preferred_element_type=jnp.float32)
                up_out[k - 1, at, :] = total.astype(jnp.bfloat16)

        @pl.when(t == rush + 1)
        def _():
            early_gradients()

        @pl.loop(t - LAG - 1 + jnp.where(t == rush + 1, 1, 0), t - LAG + jnp.where(t == rush, 1, 0))
        def _(turn):
            @pl.when(turn >= 0)
            def _():
                compute(turn)

        @pl.when(t == home_turn + 1)
        def _():
            for k in range(1, n):
                up_copy(k - 1, e).start()

        @pl.when(t + ahead < chunks)
        def _():
            to_expert(t + ahead)

    forward_across(final)
    if rush + 1 >= steady:
        early_gradients()

    @pl.loop(final if rush == steady - 1 else final - 1, chunks)
    def _(turn):
        compute(turn)

    for k in range(1, n):
        all_of(up_in.at[k - 1], u_recv.at[k - 1])

    all_of(sendbuf.at[:, pl.ds(0, experts - 1)], z_send.at[0])
    all_of(sendbuf, y_send.at[0])
    all_of(routed.at[:, :, pl.ds(0, 2)], c_send.at[0])
    all_of(cot_in, x_send.at[0])
    for k in range(1, n):
        ids_copy(k).wait_send()
        weights_copy(k).wait_send()
        product_copy(k).wait_send()
        all_of(up_out.at[k - 1], u_send.at[k - 1])


def down_gradient(routed, product, own, j, shares, total):
    rows_all = product.shape[1]
    width = routed.shape[-1]
    for k in shares:
        rows = routed[k * own + j].reshape(rows_all, width)
        total = total + lax.dot_general(
            rows, product[k], (((0,), (0,)), ((), ())), preferred_element_type=jnp.float32
        )
    return total


def finish(
    wgrad_ref,
    routed,
    product,
    upstream,
    up_in,
    slope,
    active,
    spare,
    wgrad_out,
    ggrad_out,
    ugrad_out,
    wgrad_last,
    ggrad_ref,
    ugrad_ref,
    stored,
):
    own = wgrad_ref.shape[0]
    n, rows_all, _ = product.shape
    piece = rows_all // 8
    copies = [
        pltpu.make_async_copy(source, to, stored.at[i])
        for i, (source, to) in enumerate(
            (
                (ggrad_ref, ggrad_out),
                (ugrad_ref, ugrad_out),
                (wgrad_last, wgrad_out.at[own - 1]),
            )
        )
    ]
    if own > 1:
        done = pl.ds(0, own - 1)
        copies.append(pltpu.make_async_copy(wgrad_ref.at[done], wgrad_out.at[done], stored.at[3]))
        copies[3].start()

    @pl.loop(0, 8)
    def _(i):
        at = pl.ds(pl.multiple_of(i * piece, 16), piece)
        total = upstream[0, at, :]
        for k in range(1, n):
            total = total + up_in[k - 1, at, :].astype(jnp.float32)
        ggrad_ref[at, :] = (total * slope[at, :]).astype(jnp.bfloat16)
        ugrad_ref[at, :] = (total * active[at, :]).astype(jnp.bfloat16)

    copies[0].start()
    copies[1].start()
    wgrad_last[...] = down_gradient(routed, product, own, own - 1, range(1), spare[...]).astype(jnp.bfloat16)
    copies[2].start()
    for copy in copies:
        copy.wait()


def chunk_width(depth):
    for width in (256, 128):
        if depth % width == 0:
            return width, True
    return depth, False


def per_device(cotangent, expert_ids, route_weights, gate_pre, up_pre, down_weight):
    n = lax.axis_size("dp")
    devices = lax.axis_size("expert")
    experts = devices // SPLIT
    rows, hidden = gate_pre.shape
    capacity = rows // devices
    cap = -(-capacity // 16) * 16
    depth = down_weight.shape[0]
    width, aligned = chunk_width(depth)
    own = depth // width
    chunks = n * own
    away = chunks - own
    if not aligned:
        cotangent = cotangent.reshape(-1, chunks, width).swapaxes(0, 1)

    def widen(a):
        if cap == capacity:
            return a
        a = a.reshape(devices, capacity, hidden)
        return jnp.pad(a, ((0, 0), (0, cap - capacity), (0, 0))).reshape(devices * cap, hidden)

    def narrow(a):
        if cap == capacity:
            return a
        return a.reshape(devices, cap, hidden)[:, :capacity].reshape(rows, hidden)

    padded = devices * cap
    tokens = expert_ids.shape[0]
    half, full = jnp.bfloat16, jnp.float32
    vmem = pl.BlockSpec(memory_space=pltpu.VMEM)
    anywhere = pl.BlockSpec(memory_space=pltpu.HBM)
    dma = pltpu.SemaphoreType.DMA
    kept = (
        pltpu.VMEM((own, width, hidden), half),
        pltpu.VMEM((chunks, experts, SPLIT, cap, width), half),
        pltpu.VMEM((n, padded, hidden), half),
        pltpu.VMEM((n, padded, hidden), full),
        pltpu.VMEM((n - 1, padded, hidden), half),
        pltpu.VMEM((padded, hidden), full),
        pltpu.VMEM((padded, hidden), full),
        pltpu.VMEM((width, hidden), full),
    )
    held = sum(
        math.prod(a.shape[:-1]) * -(-a.shape[-1] // 128) * 128 * jnp.dtype(a.dtype).itemsize for a in kept
    )
    parts = pl.pallas_call(
        functools.partial(kernel, (n, experts, cap, chunks, width, aligned)),
        out_shape=kept,
        in_specs=[anywhere] * 6,
        out_specs=(vmem,) * len(kept),
        scratch_shapes=[
            pltpu.VMEM(cotangent.shape, half),
            pltpu.VMEM((1, tokens), jnp.int32),
            pltpu.VMEM((1, tokens), full),
            pltpu.VMEM((padded, hidden), half),
            pltpu.VMEM((padded, hidden), half),
            pltpu.VMEM((own, width, hidden), half),
            dma((5 + n,)),
            pltpu.VMEM((chunks, experts, cap, width), half),
            pltpu.VMEM((away, tokens, width), half),
            pltpu.VMEM((n - 1, 1, tokens), jnp.int32),
            pltpu.VMEM((n - 1, 1, tokens), full),
            pltpu.VMEM((n - 1, padded, hidden), half),
            pltpu.VMEM((n, experts * cap, tokens), half),
            pltpu.VMEM((n, experts * cap, 1), full),
            dma((1,)),
            dma((min(RING, chunks) + experts - 2,)),
            dma((1,)),
            dma((min(RING, chunks) + 2,)),
            dma((1,)),
            dma((min(RING, chunks) + 2,)),
            dma((1,)),
            dma((away,)),
            dma((n - 1, 2)),
            dma((n - 1, 2)),
            dma((n - 1,)),
            dma((n - 1,)),
            dma((n - 1,)),
            dma((n - 1,)),
        ],
        compiler_params=pltpu.CompilerParams(
            collective_id=0, has_side_effects=True, vmem_limit_bytes=VMEM_BYTES - held
        ),
    )(
        cotangent,
        expert_ids.reshape(1, -1),
        route_weights.reshape(1, -1),
        widen(gate_pre),
        widen(up_pre),
        down_weight.reshape(own, width, hidden),
    )
    weight_grad, gate_grad, up_grad = pl.pallas_call(
        finish,
        out_shape=(
            jax.ShapeDtypeStruct((own, width, hidden), half),
            jax.ShapeDtypeStruct((padded, hidden), half),
            jax.ShapeDtypeStruct((padded, hidden), half),
        ),
        in_specs=[vmem] * len(kept),
        out_specs=[anywhere] * 3,
        scratch_shapes=[
            pltpu.VMEM((width, hidden), half),
            pltpu.VMEM((padded, hidden), half),
            pltpu.VMEM((padded, hidden), half),
            dma((4,)),
        ],
        compiler_params=pltpu.CompilerParams(vmem_limit_bytes=LAST_LIMIT),
    )(*parts)
    weight_grad = weight_grad.reshape(depth, hidden)
    return weight_grad, narrow(gate_grad), narrow(up_grad)


def solution(mesh):
    placed = (
        P(("dp", "expert"), None),
        P(("dp", "expert"), None),
        P(("dp", "expert"), None),
        P("dp", "expert"),
        P("dp", "expert"),
        P("dp", "expert"),
    )
    return jax.shard_map(
        per_device,
        mesh=mesh,
        in_specs=placed,
        out_specs=(P("dp", "expert"), P("dp", "expert"), P("dp", "expert")),
        check_vma=False,
    )
```

```python
import functools
import math

import jax
import jax.numpy as jnp
from jax import lax
from jax.experimental import pallas as pl
from jax.experimental.pallas import tpu as pltpu
from jax.sharding import PartitionSpec as P

SPLIT = 4
EARLY = 2
BUILD = 3
LAG = 2
RING = 6
VMEM_BYTES = 66400000
LAST_LIMIT = 12 << 20


def kernel(
    sizes,
    cot_hbm,
    ids_hbm,
    weights_hbm,
    gate_hbm,
    up_hbm,
    down_hbm,
    wgrad_ref,
    routed,
    product,
    upstream,
    up_in,
    slope,
    active,
    spare,
    cot_ref,
    ids_ref,
    weights_ref,
    gate_ref,
    up_ref,
    down_ref,
    load,
    sendbuf,
    cot_in,
    ids_in,
    weights_in,
    up_out,
    picker,
    scale,
    z_send,
    z_recv,
    y_send,
    y_recv,
    c_send,
    c_recv,
    x_send,
    x_recv,
    i_send,
    i_recv,
    p_send,
    p_recv,
    u_send,
    u_recv,
):
    n, experts, cap, chunks, width, aligned = sizes
    own = chunks // n
    away = chunks - own
    early = min(EARLY, own - 1)
    ahead = min(BUILD, chunks)
    home_turn = max(0, early + away - ahead) + 1
    block = SPLIT * cap
    final = chunks - 1
    rush = early + away + 1
    steady = final + LAG
    tokens = ids_ref.shape[1]
    dp = lax.axis_index("dp")
    me = lax.axis_index("expert")
    e, lane = me // SPLIT, me % SPLIT
    across = me - lane + (lane + 2) % SPLIT
    beside = me - lane + (lane // 2) * 2 + (lane + 1) % 2
    lane_across = (lane + 2) % SPLIT
    paired = experts & (experts - 1) == 0
    steps = sorted(range(1, experts), key=lambda k: -(k.bit_length()))
    ring = min(RING, chunks)

    def partner(k):
        if not paired:
            return (e + k) % experts
        there = e
        for bit in range(k.bit_length()):
            if k >> bit & 1:
                there = there + (1 << bit) - (2 << bit) * (e // (1 << bit) % 2)
        return there

    def origin(k):
        return partner(k) if paired else (e + experts - k) % experts

    def share_of(ref, share):
        if aligned:
            return ref.at[:, pl.ds(pl.multiple_of(share * own * width, 128), own * width)]
        return ref.at[pl.ds(share * own, own)]

    loads = [
        pltpu.make_async_copy(source, to, load.at[i])
        for i, (source, to) in enumerate(
            (
                (ids_hbm, ids_ref),
                (weights_hbm, weights_ref),
                (share_of(cot_hbm, dp), share_of(cot_ref, dp)),
                (gate_hbm, gate_ref),
                (up_hbm, up_ref),
                (down_hbm, down_ref),
            )
        )
    ]
    others = [
        pltpu.make_async_copy(
            share_of(cot_hbm, (dp + k) % n), share_of(cot_ref, (dp + k) % n), load.at[5 + k]
        )
        for k in range(1, n)
    ]
    for copy in loads[:3] + others:
        copy.start()

    barrier = pltpu.get_barrier_semaphore()

    def greet(target):
        pl.semaphore_signal(
            barrier, inc=1, device_id=target, device_id_type=pl.DeviceIdType.MESH
        )

    for k in steps:
        greet({"expert": partner(k) * SPLIT + lane})
    greet({"expert": across})
    greet({"expert": beside})
    for k in range(1, n):
        greet({"dp": (dp + k) % n})

    def send(source, to, sent, arrived, device):
        return pltpu.make_async_remote_copy(
            src_ref=source,
            dst_ref=to,
            send_sem=sent,
            recv_sem=arrived,
            device_id=device,
            device_id_type=pl.DeviceIdType.MESH,
        )

    def chunk_at(t):
        late = jnp.where(t < early + away, own - early, -away)
        return t + jnp.where(t < early, 0, late)

    def columns_of(share, j):
        if aligned:
            return cot_ref.at[:, pl.ds(pl.multiple_of((share * own + j) * width, 128), width)]
        return cot_ref.at[share * own + j]

    def cot_copy(i):
        to = (dp - 1 - i // own + n) % n
        return send(columns_of(to, i % own), cot_in.at[i], x_send.at[0], x_recv.at[i], {"dp": to})

    def ids_copy(k):
        return send(
            ids_ref, ids_in.at[k - 1], i_send.at[k - 1, 0], i_recv.at[k - 1, 0], {"dp": (dp - k + n) % n}
        )

    def weights_copy(k):
        return send(
            weights_ref, weights_in.at[k - 1], i_send.at[k - 1, 1], i_recv.at[k - 1, 1], {"dp": (dp - k + n) % n}
        )

    def product_copy(k):
        return send(
            product.at[0], product.at[k], p_send.at[k - 1], p_recv.at[k - 1], {"dp": (dp - k + n) % n}
        )

    def up_copy(i, plane):
        at = pl.ds(pl.multiple_of(plane * block, 16), block)
        return send(
            up_out.at[i, at], up_in.at[i, at], u_send.at[i], u_recv.at[i], {"dp": (dp + 1 + i) % n}
        )

    def pick(k, ids_row, weight_row):
        shape = (tokens, tokens)
        first = lax.broadcasted_iota(jnp.int32, shape, 0)
        second = lax.broadcasted_iota(jnp.int32, shape, 1)
        names = lax.broadcasted_iota(jnp.int32, (-(-experts // 16) * 16, tokens), 0) == ids_row
        before = jnp.where(first < second, 1.0, 0.0).astype(jnp.bfloat16)
        earlier = jnp.dot(
            jnp.where(names, 1.0, 0.0).astype(jnp.bfloat16), before, preferred_element_type=jnp.float32
        )
        position = jnp.sum(jnp.where(names, earlier, 0.0), axis=0, keepdims=True).astype(jnp.int32)
        target = ids_row * cap + position
        chosen = lax.broadcasted_iota(jnp.int32, (experts * cap, tokens), 0) == target
        picker[k] = jnp.where(chosen, 1.0, 0.0).astype(jnp.bfloat16)
        scale[k] = jnp.sum(jnp.where(chosen, weight_row, 0.0), axis=1, keepdims=True)

    def place(q, k, columns):
        picked = jnp.dot(picker[k], columns, preferred_element_type=jnp.float32)
        rows = (picked * scale[k]).astype(jnp.bfloat16).reshape(experts, cap, width)
        sendbuf[q] = rows
        routed[q, e, lane] = sendbuf[q, e]

    def build(t):
        q = chunk_at(t)

        @pl.when(q >= own)
        def _():
            cot_copy(q - own).wait_recv()
            place(q, q // own, cot_in[q - own])

    def to_across(q, plane, arrived):
        at = routed.at[q, plane, lane]
        send(at, at, y_send.at[0], arrived, {"expert": across}).start()

    def to_beside(at, arrived):
        send(at, at, c_send.at[0], arrived, {"expert": beside}).start()

    def forward_across(t):
        q = chunk_at(t)
        all_of(routed.at[q, pl.ds(0, experts - 1), 0], y_recv.at[t % ring])
        for k in steps:
            to_beside(routed.at[q, origin(k), lane_across], c_recv.at[t % ring])

    def to_plane(source, to, there, arrived):
        send(source, to, z_send.at[0], arrived, {"expert": there * SPLIT + lane}).start()

    def z_arrived(t, i):
        return z_recv.at[jnp.where(t == final, ring + i - 1, t % ring)] if i else z_recv.at[t % ring]

    def to_expert(t):
        q = chunk_at(t)
        for i, k in enumerate(steps):
            there = partner(k)
            to_plane(sendbuf.at[q, there], routed.at[q, e, lane], there, z_arrived(t, i))

        @pl.when(q >= own)
        def _():
            to_across(q, e, y_recv.at[ring + 1])

    def all_of(ref_at, sem):
        pltpu.make_async_copy(ref_at, ref_at, sem).wait()

    def forward(t, k):
        q, plane = chunk_at(t), origin(k)
        to_across(q, plane, y_recv.at[t % ring])
        to_beside(routed.at[q, plane, lane], c_recv.at[t % ring])

    loads[0].wait()
    loads[1].wait()
    pick(0, ids_ref[...], weights_ref[...])
    loads[2].wait()
    for j in range(early):
        place(j, 0, columns_of(dp, j)[...])
    pl.semaphore_wait(barrier, experts - 1 + 2 + n - 1)
    for j in range(early):
        to_expert(j)
    for k in range(1, n):
        ids_copy(k).start()
        weights_copy(k).start()
    for copy in others:
        copy.wait()

    @pl.loop(0, away)
    def _(i):
        cot_copy(i).start()

    for copy in loads[3:]:
        copy.start()
    for j in range(early):
        to_across(j, e, y_recv.at[ring])

    @pl.loop(early, own)
    def _(j):
        place(j, 0, columns_of(dp, j)[...])

    rows_all = gate_ref.shape[0]
    piece = rows_all // 8
    loads[3].wait()
    loads[4].wait()

    @pl.loop(0, 8)
    def _(i):
        at = pl.ds(pl.multiple_of(i * piece, 16), piece)
        gate = gate_ref[at, :].astype(jnp.float32)
        up = up_ref[at, :].astype(jnp.float32)
        sig = jax.nn.sigmoid(gate)
        act = gate * sig
        active[at, :] = act
        slope[at, :] = up * sig * (1.0 + gate * (1.0 - sig))
        product[0, at, :] = (act * up).astype(jnp.bfloat16)
        for k in range(n):
            upstream[k, at, :] = jnp.zeros_like(act)

    @pl.loop(early, own)
    def _(j):
        to_across(j, e, y_recv.at[ring])

    to_beside(routed.at[pl.ds(0, own), e, lane], c_recv.at[ring])

    for k in range(1, n):
        ids_copy(k).wait_recv()
        weights_copy(k).wait_recv()
        pick(k, ids_in[k - 1], weights_in[k - 1])
    for t in range(early, ahead):
        build(t)
    for k in range(1, n):
        product_copy(k).start()
    loads[5].wait()
    for t in range(early, ahead):
        to_expert(t)

    edge = (e == 0) | (e == experts - 1)

    def gradient(j):
        total = jnp.zeros((width, product.shape[2]), jnp.float32)
        wgrad_ref[j] = down_gradient(routed, product, own, j, range(n), total).astype(jnp.bfloat16)

    def compute(turn):
        q = chunk_at(turn)
        k, j = q // own, q % own

        @pl.when(turn == 0)
        def _():
            all_of(routed.at[pl.ds(0, own), 0, pl.ds(0, 2)], c_recv.at[ring])

        all_of(routed.at[q, pl.ds(0, experts - 1), pl.ds(0, 2)], c_recv.at[turn % ring])

        @pl.when(k == 0)
        def _():
            rows = routed[q].reshape(rows_all, width)
            upstream[0] += jnp.dot(rows, down_ref[j], preferred_element_type=jnp.float32)

        @pl.when(k >= 1)
        def _():
            for step in steps:
                plane = origin(step)
                at = pl.ds(pl.multiple_of(plane * block, 16), block)
                rows = routed[q, plane].reshape(block, width)
                upstream[k, at, :] += jnp.dot(rows, down_ref[j], preferred_element_type=jnp.float32)

                @pl.when(j == own - 1)
                def _():
                    up_out[k - 1, at, :] = upstream[k, at, :].astype(jnp.bfloat16)

        @pl.when((turn >= early + away) & (turn < final))
        def _():
            gradient(j)

        @pl.when((k >= 1) & (j == own - 1))
        def _():
            for step in steps:
                up_copy(k - 1, origin(step)).start()

    def early_gradients():
        for k in range(1, n):
            product_copy(k).wait_recv()
        for j in range(early):
            gradient(j)
        total = jnp.zeros((width, product.shape[2]), jnp.float32)
        spare[...] = down_gradient(routed, product, own, own - 1, range(1, n), total)

    @pl.loop(0, steady)
    def _(t):
        @pl.when(t >= LAG)
        def _():
            @pl.when(t == LAG)
            def _():
                all_of(routed.at[pl.ds(0, own), 0, 0], y_recv.at[ring])
                to_beside(routed.at[pl.ds(0, own), e, lane_across], c_recv.at[ring])

            forward_across(t - LAG)

        @pl.when(edge & (t >= 1) & (t + ahead - 1 >= early + away) & (t + ahead - 1 < chunks))
        def _():
            to_expert(t + ahead - 1)

        @pl.when(t < final)
        def _():
            all_of(routed.at[0, pl.ds(0, experts - 1), 0], z_recv.at[t % ring])
            for k in steps:
                forward(t, k)

        @pl.when(t == final)
        def _():
            for i, k in enumerate(steps):
                all_of(routed.at[own - 1, 0, 0], z_arrived(final, i))
                forward(final, k)

        @pl.when(t + ahead < early + away)
        def _():
            build(t + ahead)

        @pl.when(t == home_turn)
        def _():
            theirs = pl.ds(own, away)
            to_beside(routed.at[theirs, e, lane], c_recv.at[ring + 1])
            all_of(routed.at[theirs, 0, 0], y_recv.at[ring + 1])
            to_beside(routed.at[theirs, e, lane_across], c_recv.at[ring + 1])

        @pl.when(t == home_turn + 1)
        def _():
            all_of(routed.at[pl.ds(own, away), 0, pl.ds(0, 2)], c_recv.at[ring + 1])
            at = pl.ds(pl.multiple_of(e * block, 16), block)
            for k in range(1, n):
                total = jnp.zeros((block, product.shape[2]), jnp.float32)
                for j in range(own):
                    rows = routed[k * own + j, e].reshape(block, width)
                    total = total + jnp.dot(rows, down_ref[j], preferred_element_type=jnp.float32)
                up_out[k - 1, at, :] = total.astype(jnp.bfloat16)

        @pl.when(t == rush + 1)
        def _():
            early_gradients()

        @pl.loop(t - LAG - 1 + jnp.where(t == rush + 1, 1, 0), t - LAG + jnp.where(t == rush, 1, 0))
        def _(turn):
            @pl.when(turn >= 0)
            def _():
                compute(turn)

        @pl.when(t == home_turn + 1)
        def _():
            for k in range(1, n):
                up_copy(k - 1, e).start()

        @pl.when((t + ahead < early + away) | ((t + ahead < chunks) & jnp.logical_not(edge)))
        def _():
            to_expert(t + ahead)

    forward_across(final)
    if rush + 1 >= steady:
        early_gradients()

    @pl.loop(final if rush == steady - 1 else final - 1, chunks)
    def _(turn):
        compute(turn)

    for k in range(1, n):
        all_of(up_in.at[k - 1], u_recv.at[k - 1])

    all_of(sendbuf.at[:, pl.ds(0, experts - 1)], z_send.at[0])
    all_of(sendbuf, y_send.at[0])
    all_of(routed.at[:, :, pl.ds(0, 2)], c_send.at[0])
    all_of(cot_in, x_send.at[0])
    for k in range(1, n):
        ids_copy(k).wait_send()
        weights_copy(k).wait_send()
        product_copy(k).wait_send()
        all_of(up_out.at[k - 1], u_send.at[k - 1])


def down_gradient(routed, product, own, j, shares, total):
    rows_all = product.shape[1]
    width = routed.shape[-1]
    for k in shares:
        rows = routed[k * own + j].reshape(rows_all, width)
        total = total + lax.dot_general(
            rows, product[k], (((0,), (0,)), ((), ())), preferred_element_type=jnp.float32
        )
    return total


def finish(
    wgrad_ref,
    routed,
    product,
    upstream,
    up_in,
    slope,
    active,
    spare,
    wgrad_out,
    ggrad_out,
    ugrad_out,
    wgrad_last,
    ggrad_ref,
    ugrad_ref,
    stored,
):
    own = wgrad_ref.shape[0]
    n, rows_all, _ = product.shape
    piece = rows_all // 8
    copies = [
        pltpu.make_async_copy(source, to, stored.at[i])
        for i, (source, to) in enumerate(
            (
                (ggrad_ref, ggrad_out),
                (ugrad_ref, ugrad_out),
                (wgrad_last, wgrad_out.at[own - 1]),
            )
        )
    ]
    if own > 1:
        done = pl.ds(0, own - 1)
        copies.append(pltpu.make_async_copy(wgrad_ref.at[done], wgrad_out.at[done], stored.at[3]))
        copies[3].start()

    @pl.loop(0, 8)
    def _(i):
        at = pl.ds(pl.multiple_of(i * piece, 16), piece)
        total = upstream[0, at, :]
        for k in range(1, n):
            total = total + up_in[k - 1, at, :].astype(jnp.float32)
        ggrad_ref[at, :] = (total * slope[at, :]).astype(jnp.bfloat16)
        ugrad_ref[at, :] = (total * active[at, :]).astype(jnp.bfloat16)

    copies[0].start()
    copies[1].start()
    wgrad_last[...] = down_gradient(routed, product, own, own - 1, range(1), spare[...]).astype(jnp.bfloat16)
    copies[2].start()
    for copy in copies:
        copy.wait()


def chunk_width(depth):
    for width in (256, 128):
        if depth % width == 0:
            return width, True
    return depth, False


def per_device(cotangent, expert_ids, route_weights, gate_pre, up_pre, down_weight):
    n = lax.axis_size("dp")
    devices = lax.axis_size("expert")
    experts = devices // SPLIT
    rows, hidden = gate_pre.shape
    capacity = rows // devices
    cap = -(-capacity // 16) * 16
    depth = down_weight.shape[0]
    width, aligned = chunk_width(depth)
    own = depth // width
    chunks = n * own
    away = chunks - own
    if not aligned:
        cotangent = cotangent.reshape(-1, chunks, width).swapaxes(0, 1)

    def widen(a):
        if cap == capacity:
            return a
        a = a.reshape(devices, capacity, hidden)
        return jnp.pad(a, ((0, 0), (0, cap - capacity), (0, 0))).reshape(devices * cap, hidden)

    def narrow(a):
        if cap == capacity:
            return a
        return a.reshape(devices, cap, hidden)[:, :capacity].reshape(rows, hidden)

    padded = devices * cap
    tokens = expert_ids.shape[0]
    half, full = jnp.bfloat16, jnp.float32
    vmem = pl.BlockSpec(memory_space=pltpu.VMEM)
    anywhere = pl.BlockSpec(memory_space=pltpu.HBM)
    dma = pltpu.SemaphoreType.DMA
    kept = (
        pltpu.VMEM((own, width, hidden), half),
        pltpu.VMEM((chunks, experts, SPLIT, cap, width), half),
        pltpu.VMEM((n, padded, hidden), half),
        pltpu.VMEM((n, padded, hidden), full),
        pltpu.VMEM((n - 1, padded, hidden), half),
        pltpu.VMEM((padded, hidden), full),
        pltpu.VMEM((padded, hidden), full),
        pltpu.VMEM((width, hidden), full),
    )
    held = sum(
        math.prod(a.shape[:-1]) * -(-a.shape[-1] // 128) * 128 * jnp.dtype(a.dtype).itemsize for a in kept
    )
    parts = pl.pallas_call(
        functools.partial(kernel, (n, experts, cap, chunks, width, aligned)),
        out_shape=kept,
        in_specs=[anywhere] * 6,
        out_specs=(vmem,) * len(kept),
        scratch_shapes=[
            pltpu.VMEM(cotangent.shape, half),
            pltpu.VMEM((1, tokens), jnp.int32),
            pltpu.VMEM((1, tokens), full),
            pltpu.VMEM((padded, hidden), half),
            pltpu.VMEM((padded, hidden), half),
            pltpu.VMEM((own, width, hidden), half),
            dma((5 + n,)),
            pltpu.VMEM((chunks, experts, cap, width), half),
            pltpu.VMEM((away, tokens, width), half),
            pltpu.VMEM((n - 1, 1, tokens), jnp.int32),
            pltpu.VMEM((n - 1, 1, tokens), full),
            pltpu.VMEM((n - 1, padded, hidden), half),
            pltpu.VMEM((n, experts * cap, tokens), half),
            pltpu.VMEM((n, experts * cap, 1), full),
            dma((1,)),
            dma((min(RING, chunks) + experts - 2,)),
            dma((1,)),
            dma((min(RING, chunks) + 2,)),
            dma((1,)),
            dma((min(RING, chunks) + 2,)),
            dma((1,)),
            dma((away,)),
            dma((n - 1, 2)),
            dma((n - 1, 2)),
            dma((n - 1,)),
            dma((n - 1,)),
            dma((n - 1,)),
            dma((n - 1,)),
        ],
        compiler_params=pltpu.CompilerParams(
            collective_id=0, has_side_effects=True, vmem_limit_bytes=VMEM_BYTES - held
        ),
    )(
        cotangent,
        expert_ids.reshape(1, -1),
        route_weights.reshape(1, -1),
        widen(gate_pre),
        widen(up_pre),
        down_weight.reshape(own, width, hidden),
    )
    weight_grad, gate_grad, up_grad = pl.pallas_call(
        finish,
        out_shape=(
            jax.ShapeDtypeStruct((own, width, hidden), half),
            jax.ShapeDtypeStruct((padded, hidden), half),
            jax.ShapeDtypeStruct((padded, hidden), half),
        ),
        in_specs=[vmem] * len(kept),
        out_specs=[anywhere] * 3,
        scratch_shapes=[
            pltpu.VMEM((width, hidden), half),
            pltpu.VMEM((padded, hidden), half),
            pltpu.VMEM((padded, hidden), half),
            dma((4,)),
        ],
        compiler_params=pltpu.CompilerParams(vmem_limit_bytes=LAST_LIMIT),
    )(*parts)
    weight_grad = weight_grad.reshape(depth, hidden)
    return weight_grad, narrow(gate_grad), narrow(up_grad)


def solution(mesh):
    placed = (
        P(("dp", "expert"), None),
        P(("dp", "expert"), None),
        P(("dp", "expert"), None),
        P("dp", "expert"),
        P("dp", "expert"),
        P("dp", "expert"),
    )
    return jax.shard_map(
        per_device,
        mesh=mesh,
        in_specs=placed,
        out_specs=(P("dp", "expert"), P("dp", "expert"), P("dp", "expert")),
        check_vma=False,
    )
```
